256 devices in a mesh: groups: 2 (over y), context: 128 (over x, z, core).
Axes of the slice: x: 4, y: 2, z: 16, core: 2. Of those that a mesh axis runs over, the one named last changes fastest.
The devices are a block of a 4x16x16 slice.
Arguments:
- query_proj: bfloat16 [32768, 5120], P(('groups', 'context')), parts along dimension 0, may hold values from -100 to 100
- key_proj: bfloat16 [32768, 1024], P(('groups', 'context')), parts along dimension 0, may hold values from -100 to 100
- values: bfloat16 [32768, 1024], P(('groups', 'context')), parts along dimension 0, may hold values from -6 to 6
- grad_out: bfloat16 [32768, 5120], P(('groups', 'context')), parts along dimension 0, may hold values from -6 to 6
- query_gain: float32 [5120], replicated, may hold values from 0.1 to 1.9
- key_gain: float32 [1024], replicated, may hold values from 0.1 to 1.9
- segments: int32 [32768], P('groups'), parts along dimension 0, may hold values from 0 to 63, never falling along the last dimension, each value on 1 to 512 neighbouring positions
- layout: int32 [512], P('groups'), parts along dimension 0, may hold values from 0 to 255, as said below
Outputs:
- query_grad: bfloat16 [32768, 5120], P(('groups', 'context')), parts along dimension 0
- key_grad: bfloat16 [32768, 1024], P(('groups', 'context')), parts along dimension 0
- value_grad: bfloat16 [32768, 1024], P(('groups', 'context')), parts along dimension 0
- query_gain_grad: float32 [10240], P('groups'), parts along dimension 0
- key_gain_grad: float32 [2048], P('groups'), parts along dimension 0
The draws below stay inside these ranges and needn't reach their ends.
There are 2 independent parts, one for each index of `groups`. The reference program is written for one: setup_inputs(seed, part) draws one part's arguments, and reference() takes and returns one part's arrays. A program takes and returns all parts, laid end to end along the dimension named above; an argument that names none is the same for every part. Nothing has to cross between parts.
Inputs may be any that keep to these rules, and one draw needn't show every extreme that they name: layout is a permutation of the spans; slots are ordered device by device, 2 to a device, and each aligned run of 8 slots holds the spans of one sequence of 512 positions in some order. `segments`: document numbers never fall along the stream; a document has 1 to 512 positions, and one has exactly 512.
All inputs are finite; a program needn't handle non-finite values.
Results may differ from the reference program's by a relative error of at most 0.0086.
Values may be sent and summed in bfloat16 or wider, within the bound.
A program may use at most 128 MiB of HBM per device.

```python
import math
import jax
import jax.numpy as jnp
import numpy as np
from jax import lax

QUERY_HEADS = 40
KEY_VALUE_HEADS = 8
HEAD_SIZE = 128
SPAN = 64
CPD = 2
SEQ_DEVS = 4
QW = 5120
KW = 1024
TOK_DEV = 128
LENGTH = 512
STREAM_TOKENS = 16384
DOCS = 64
N_CONTEXT = 128


def draw_layout(key, part):
    window = SEQ_DEVS * CPD
    slot_count = STREAM_TOKENS // SPAN
    own_key = jax.random.fold_in(key, 3)
    scores = jax.random.randint(own_key, (slot_count // window, window), 0, 65536) * window + jnp.arange(window, dtype=jnp.int32)[None, :]
    local_order = jnp.argsort(scores, axis=1).astype(jnp.int32)
    starts = jnp.arange(slot_count // window, dtype=jnp.int32)[:, None] * window
    return (local_order + starts).reshape(slot_count).astype(jnp.int32)


def projection_sample(key, salt, width):
    own_key = jax.random.fold_in(key, salt)
    return jnp.clip(jax.random.normal(own_key, (STREAM_TOKENS, width)), -8.0, 8.0).astype(jnp.bfloat16)


def draw_query_proj(key, part):
    return projection_sample(key, 11, QUERY_HEADS * HEAD_SIZE)


def draw_key_proj(key, part):
    return projection_sample(key, 13, KEY_VALUE_HEADS * HEAD_SIZE)


def block_scale(rng, extent, split, low, top_value):
    loudness = 1.0
    for position, shards_of in split:
        steps = jax.random.uniform(jax.random.fold_in(jax.random.fold_in(rng, 6), position), (shards_of,), jnp.float32, low / len(split), top_value / len(split))
        loudness = loudness * jnp.repeat(jnp.exp(steps), extent[position] // shards_of).reshape((-1,) + (1,) * (len(extent) - 1 - position))
    return loudness


def split_up(amount, total, bound, slope):
    loads = [(1 << 20) // math.isqrt(standing ** slope) + 1 for standing in range(2, amount + 1)]
    rest, given = total - bound - (amount - 1), [1] * (amount - 1)
    while rest > 0:
        candidates = [i for i in range(amount - 1) if given[i] < bound]
        whole, budget = sum([loads[i] for i in candidates]), rest
        for i in candidates:
            more = min(bound - given[i], max(1, budget * loads[i] // whole), rest)
            given[i] = given[i] + more
            rest = rest - more
    return np.array([bound] + given)


def uneven_parts(rng, count, total, most, slope):
    if count == 2:
        one = jax.random.randint(rng, (), max(1, total - most), min(most, total - 1) + 1)
        return jnp.stack([one, total - one])
    lengths = jnp.asarray(split_up(count, total, most, slope), jnp.int32)
    twos = (count - 1) // 2
    giver, taker = lengths[1:1 + 2 * twos:2], lengths[2:2 + 2 * twos:2]
    room = jnp.minimum(giver - 1, most - taker)
    moved = jax.random.randint(jax.random.fold_in(rng, 1), (twos,), 0, 1 << 20) % (room + 1)
    lengths = lengths.at[1:1 + 2 * twos:2].set(giver - moved).at[2:2 + 2 * twos:2].set(taker + moved)
    return lengths[jax.random.permutation(jax.random.fold_in(rng, 2), count)]


def noise(key, shape, deviation, most, shards=(), kind=jnp.bfloat16):
    drawn = jax.random.normal(key, shape, jnp.float32) * deviation
    if len(shards) > 0:
        drawn = block_scale(key, shape, shards, -0.22, 0.18) * drawn
    return jnp.clip(drawn, min=-most, max=most).astype(kind)


def setup_inputs(seed: int = 0, part: int = 0) -> dict:
    keys = jax.random.split(jax.random.key(seed), 9)
    part_keys = jax.random.split(jax.random.fold_in(keys[8], part), 9)
    query_proj = draw_query_proj(jax.random.fold_in(jax.random.fold_in(keys[8], part), 71), part)
    key_proj = draw_key_proj(jax.random.fold_in(jax.random.fold_in(keys[8], part), 71), part)
    values = noise(part_keys[2], (STREAM_TOKENS, KW), 1.0, 6.0, ((0, 128),))
    grad_out = noise(part_keys[3], (STREAM_TOKENS, QW), 1.0, 6.0, ((0, 128),))
    query_gain = jnp.clip(1.0 + 0.18 * jax.random.normal(keys[4], (QW,), jnp.float32), 0.1, 1.9)
    key_gain = jnp.clip(1.0 + 0.18 * jax.random.normal(keys[5], (KW,), jnp.float32), 0.1, 1.9)
    segments = jnp.searchsorted(jnp.cumsum(uneven_parts(part_keys[6], DOCS, STREAM_TOKENS, LENGTH, 2)), jnp.arange(STREAM_TOKENS), side="right").astype(jnp.int32)
    layout = draw_layout(jax.random.fold_in(jax.random.fold_in(keys[8], part), 71), part)
    return {"query_proj": query_proj, "key_proj": key_proj, "values": values, "grad_out": grad_out, "query_gain": query_gain, "key_gain": key_gain, "segments": segments, "layout": layout}


NORM_EPS = 1e-06
ROPE_BASE = 500000.0

def rope_angles(positions, head_dim):
    half_dim = head_dim // 2
    inv_freq = jnp.power(ROPE_BASE, -2.0 * jnp.arange(half_dim, dtype=jnp.float32) / head_dim)
    angles = positions.astype(jnp.float32)[:, None] * inv_freq[None, :]
    return (jnp.cos(angles), jnp.sin(angles))

def rotate(inputs, cosine, sine, sign_flip):
    tok_rows = inputs.shape[0]
    half_dim = cosine.shape[1]
    halves = inputs.reshape(tok_rows, inputs.shape[1] // (2 * half_dim), 2, half_dim)
    lower_half = halves[:, :, 0]
    upper_half = halves[:, :, 1]
    cosine_b = cosine[:, None, :]
    sine_b = sine[:, None, :] * sign_flip
    rotated = jnp.stack([lower_half * cosine_b - upper_half * sine_b, upper_half * cosine_b + lower_half * sine_b], axis=2)
    return rotated.reshape(tok_rows, inputs.shape[1])

def norm_forward(inputs, gain_row):
    mean_sq = lax.optimization_barrier(jnp.mean(inputs * inputs, axis=1, keepdims=True))
    factor = lax.rsqrt(mean_sq + NORM_EPS)
    return (inputs * factor * gain_row[None, :], factor)

def norm_backward(inputs, factor, gain_row, upstream):
    weighted = upstream * gain_row[None, :]
    inner_sum = lax.optimization_barrier(jnp.mean(weighted * inputs, axis=1, keepdims=True))
    grad_in = factor * weighted - inputs * factor * factor * factor * inner_sum
    return (grad_in, lax.optimization_barrier(jnp.sum(upstream * inputs * factor, axis=0)))

def head_gradients(queries, key_rows, value_rows, grad_rows, allowed, query_head_group, head_dim):
    tok_rows = queries.shape[0]
    factor = head_dim ** (-0.5)
    query_heads = queries.reshape(tok_rows, query_head_group, head_dim).astype(jnp.float32)
    grad_heads = grad_rows.reshape(tok_rows, query_head_group, head_dim).astype(jnp.float32)
    key_float = key_rows.astype(jnp.float32)
    value_float = value_rows.astype(jnp.float32)
    scores = jnp.einsum('qgd,kd->gqk', query_heads, key_float) * factor
    scores = jnp.where(allowed[None], scores, -jnp.inf)
    row_max = lax.optimization_barrier(jnp.max(scores, axis=2, keepdims=True))
    expo = jnp.exp(scores - row_max)
    attn_probs = expo / lax.optimization_barrier(jnp.sum(expo, axis=2, keepdims=True))
    dprobs = jnp.einsum('qgd,kd->gqk', grad_heads, value_float)
    row_delta = lax.optimization_barrier(jnp.sum(attn_probs * dprobs, axis=2, keepdims=True))
    dscores = (attn_probs * (dprobs - row_delta)).astype(jnp.bfloat16).astype(jnp.float32)
    probs_low = attn_probs.astype(jnp.bfloat16).astype(jnp.float32)
    query_part = jnp.einsum('gqk,kd->qgd', dscores, key_float) * factor
    key_part = jnp.einsum('gqk,qgd->kd', dscores, query_heads) * factor
    value_part = jnp.einsum('gqk,qgd->kd', probs_low, grad_heads)
    return (query_part.reshape(tok_rows, query_head_group * head_dim), key_part, value_part)

def reference(query_proj, key_proj, values, grad_out, query_gain, key_gain, segments, layout):
    query_head_group = QUERY_HEADS // KEY_VALUE_HEADS
    group_width = query_head_group * HEAD_SIZE
    token_index = jnp.arange(STREAM_TOKENS, dtype=jnp.int32)
    positions = (jnp.take(layout, token_index // SPAN) * SPAN + token_index % SPAN).astype(jnp.int32)
    doc_ids = jnp.take(segments, positions)
    cosine, sine = rope_angles(positions % LENGTH, HEAD_SIZE)
    q_inputs = query_proj.astype(jnp.float32)
    k_inputs = key_proj.astype(jnp.float32)
    q_normed, q_factor = norm_forward(q_inputs, query_gain)
    k_normed, k_factor = norm_forward(k_inputs, key_gain)
    q_rope = rotate(q_normed, cosine, sine, 1.0).astype(jnp.bfloat16)
    k_rope = rotate(k_normed, cosine, sine, 1.0).astype(jnp.bfloat16)

    def block_step(carried, device):
        dk_acc, dv_acc = carried
        q_start = (device * TOK_DEV).astype(jnp.int32)
        k_start = (device // SEQ_DEVS * LENGTH).astype(jnp.int32)
        q_block = lax.dynamic_slice_in_dim(q_rope, q_start, TOK_DEV, 0)
        g_block = lax.dynamic_slice_in_dim(grad_out, q_start, TOK_DEV, 0)
        k_block = lax.dynamic_slice_in_dim(k_rope, k_start, LENGTH, 0)
        v_block = lax.dynamic_slice_in_dim(values, k_start, LENGTH, 0)
        pos_query = lax.dynamic_slice_in_dim(positions, q_start, TOK_DEV, 0)
        doc_query = lax.dynamic_slice_in_dim(doc_ids, q_start, TOK_DEV, 0)
        pos_key = lax.dynamic_slice_in_dim(positions, k_start, LENGTH, 0)
        doc_key = lax.dynamic_slice_in_dim(doc_ids, k_start, LENGTH, 0)
        same_seq = pos_key[None, :] // LENGTH == pos_query[:, None] // LENGTH
        allowed = same_seq & (doc_key[None, :] == doc_query[:, None]) & (pos_key[None, :] <= pos_query[:, None])
        query_parts, key_parts, value_parts = ([], [], [])
        for key_value_head in range(KEY_VALUE_HEADS):
            query_part, key_part, value_part = head_gradients(q_block[:, key_value_head * group_width:(key_value_head + 1) * group_width], k_block[:, key_value_head * HEAD_SIZE:(key_value_head + 1) * HEAD_SIZE], v_block[:, key_value_head * HEAD_SIZE:(key_value_head + 1) * HEAD_SIZE], g_block[:, key_value_head * group_width:(key_value_head + 1) * group_width], allowed, query_head_group, HEAD_SIZE)
            query_parts.append(query_part)
            key_parts.append(key_part)
            value_parts.append(value_part)
        key_block_grad = jnp.concatenate(key_parts, axis=1)
        value_block_grad = jnp.concatenate(value_parts, axis=1)
        dk_acc = lax.dynamic_update_slice_in_dim(dk_acc, lax.dynamic_slice_in_dim(dk_acc, k_start, LENGTH, 0) + key_block_grad, k_start, 0)
        dv_acc = lax.dynamic_update_slice_in_dim(dv_acc, lax.dynamic_slice_in_dim(dv_acc, k_start, LENGTH, 0) + value_block_grad, k_start, 0)
        return ((dk_acc, dv_acc), jnp.concatenate(query_parts, axis=1))
    key_zeros = jnp.zeros((STREAM_TOKENS, KEY_VALUE_HEADS * HEAD_SIZE), jnp.float32)
    (dk_rope, dv_sum), dq_blocks = lax.scan(block_step, (key_zeros, key_zeros), jnp.arange(N_CONTEXT, dtype=jnp.int32))
    dq_rope = dq_blocks.reshape(STREAM_TOKENS, QUERY_HEADS * HEAD_SIZE)
    dq_normed = rotate(dq_rope, cosine, sine, -1.0)
    dk_normed = rotate(dk_rope, cosine, sine, -1.0)
    query_grad, query_gain_grad = norm_backward(q_inputs, q_factor, query_gain, dq_normed)
    key_grad, key_gain_grad = norm_backward(k_inputs, k_factor, key_gain, dk_normed)
    return (query_grad.astype(jnp.bfloat16), key_grad.astype(jnp.bfloat16), dv_sum.astype(jnp.bfloat16), query_gain_grad, key_gain_grad)
```

```python
import functools
import math

import jax
import jax.numpy as jnp
import numpy as np
from jax import lax
from jax.experimental import pallas as pl
from jax.experimental.pallas import tpu as pltpu
from jax.sharding import Mesh
from jax.sharding import PartitionSpec as P

QUERY_HEADS = 40
KEY_VALUE_HEADS = 8
HEADS_PER = QUERY_HEADS // KEY_VALUE_HEADS
HEAD_SIZE = 128
SPAN = 64
LENGTH = 512
SPANS = LENGTH // SPAN
TOK = 128
QROWS = HEADS_PER * TOK
CONTEXT = ("context_0", "context_1", "context_2")
GROUPS_CONTEXT = ("groups", "context_0", "context_1", "context_2")
NORM_EPS = 1e-06
ROPE_BASE = 500000.0
SCALE = HEAD_SIZE ** (-0.5)
SCALE2 = SCALE * math.log2(math.e)
MESH = pl.DeviceIdType.MESH
F32 = jnp.float32
BF16 = jnp.bfloat16


def rope_tables():
    half = HEAD_SIZE // 2
    inv_freq = np.power(ROPE_BASE, -2.0 * np.arange(half) / HEAD_SIZE)
    angles = np.arange(LENGTH)[:, None] * inv_freq[None, :]
    cosine, sine = np.cos(angles), np.sin(angles)
    return (
        np.concatenate([cosine, cosine], axis=1).astype(np.float32),
        np.concatenate([-sine, sine], axis=1).astype(np.float32),
    )


def swap_halves(x):
    return pltpu.roll(x, HEAD_SIZE // 2, 1)


def kernel(
    nx, nz, nc,
    q_hbm, k_hbm, v_hbm, g_hbm, qg_ref, kg_ref, seg_ref, cos_ref, sin_ref, lay_ref,
    qgrad_hbm, kgrad_hbm, vgrad_hbm, qgain_ref, kgain_ref,
    q_vm, g_vm, k_vm, kv, qr, st, dp, pt, ds, dqw, dkw,
    bias, segcol, cosk, sink, rqb, rkb, inner,
    own, mid, sd, rd, si, ri, outb,
    gpart, rs, zb, ag,
    in_sem, kin_sem, vin_sem,
    z_send, z_recv, c_send, c_recv, f_send, f_recv,
    d_send, d_recv, i_send, i_recv,
    rs_send, rs_recv, zb_send, zb_recv, ag_send, ag_recv, out_sem,
):
    xi = lax.axis_index("context_0")
    zi = lax.axis_index("context_1")
    ci = lax.axis_index("context_2")
    rank = xi * nc + ci
    seq = xi * (nz // 2) + zi // 2
    z_flip = zi + 1 - 2 * lax.rem(zi, 2)
    partner = {"context_2": 1 - ci}
    across = {"context_1": z_flip}

    def rank_peer(other):
        return {"context_0": other // nc, "context_2": lax.rem(other, nc)}

    def k_in(h):
        cols = pl.ds(pl.multiple_of(h * HEAD_SIZE, HEAD_SIZE), HEAD_SIZE)
        return pltpu.make_async_copy(k_hbm.at[:, cols], k_vm.at[h], kin_sem.at[h])

    def v_in(h):
        cols = pl.ds(pl.multiple_of(h * HEAD_SIZE, HEAD_SIZE), HEAD_SIZE)
        return pltpu.make_async_copy(v_hbm.at[:, cols], kv.at[h, 1, 0:TOK], vin_sem.at[h])

    def q_in(h, j):
        cols = pl.ds(pl.multiple_of((h * HEADS_PER + j) * HEAD_SIZE, HEAD_SIZE), HEAD_SIZE)
        rows = pl.ds(j * TOK, TOK)
        return pltpu.make_async_copy(q_hbm.at[:, cols], q_vm.at[h, rows], in_sem.at[0, h, j])

    def g_in(h, j):
        cols = pl.ds(pl.multiple_of((h * HEADS_PER + j) * HEAD_SIZE, HEAD_SIZE), HEAD_SIZE)
        rows = pl.ds(j * TOK, TOK)
        return pltpu.make_async_copy(g_hbm.at[:, cols], g_vm.at[h, rows], in_sem.at[1, h, j])

    @pl.loop(0, KEY_VALUE_HEADS)
    def _(h):
        k_in(h).start()
        v_in(h).start()

    @pl.loop(0, KEY_VALUE_HEADS)
    def _(h):
        for j in range(HEADS_PER):
            q_in(h, j).start()
            g_in(h, j).start()

    barrier = pltpu.get_barrier_semaphore()
    for d in range(1, nx * nc):
        pl.semaphore_signal(
            barrier, inc=1, device_id=rank_peer(jnp.bitwise_xor(rank, d)), device_id_type=MESH
        )
    for d in range(1, nz):
        pl.semaphore_signal(
            barrier, inc=1, device_id={"context_1": lax.rem(zi + d, nz)}, device_id_type=MESH
        )

    my_local = 2 * lax.rem(zi, 2) + ci
    sub_iota = lax.broadcasted_iota(jnp.int32, (SPAN, TOK), 0)
    lane = lax.broadcasted_iota(jnp.int32, (8, TOK), 1)
    spans = []
    for flip in (0, 2, 1, 3):
        holder = jnp.bitwise_xor(my_local, flip)
        for part in range(2):
            slot = lay_ref[seq * SPANS + 2 * holder + part]
            spans.append(jnp.bitwise_and(jnp.full((8, TOK), slot, jnp.int32), SPANS - 1))

    def pick(span, table):
        chosen = table[0:SPAN, :]
        wide = jnp.concatenate([span] * (SPAN // 8), axis=0)
        for at in range(1, SPANS):
            chosen = jnp.where(wide == at, table[at * SPAN : (at + 1) * SPAN, :], chosen)
        return chosen

    for index, span in enumerate(spans):
        rows = slice(index * SPAN, (index + 1) * SPAN)
        cosk[rows, :] = pick(span, cos_ref)
        sink[rows, :] = pick(span, sin_ref)

    @pl.loop(0, KEY_VALUE_HEADS)
    def _(h):
        k_in(h).wait()

    acc = jnp.zeros((TOK, HEAD_SIZE), F32)
    for h in range(KEY_VALUE_HEADS):
        x = k_vm[h].astype(F32)
        acc = acc + x * x
    mean_sq = jnp.sum(acc, axis=1, keepdims=True) * (1.0 / (KEY_VALUE_HEADS * HEAD_SIZE))
    rkb[...] = jnp.broadcast_to(lax.rsqrt(mean_sq + NORM_EPS), (TOK, HEAD_SIZE))

    @pl.loop(0, KEY_VALUE_HEADS)
    def _(h):
        x = k_vm[h].astype(F32)
        normed = x * rkb[...] * kg_ref[pl.ds(h, 1), :]
        kv[h, 0, 0:TOK] = (normed * cosk[0:TOK] + swap_halves(normed) * sink[0:TOK]).astype(BF16)
        v_in(h).wait()

    pl.semaphore_wait(barrier, nx * nc - 1 + nz - 1)

    def to_across(h):
        return pltpu.make_async_remote_copy(
            kv.at[h, :, 0:TOK], kv.at[h, :, TOK : 2 * TOK], z_send.at[h], z_recv.at[h],
            device_id=across, device_id_type=MESH,
        )

    def to_partner(h):
        return pltpu.make_async_remote_copy(
            kv.at[h, :, 0:TOK], kv.at[h, :, 2 * TOK : 3 * TOK], c_send.at[h], c_recv.at[h],
            device_id=partner, device_id_type=MESH,
        )

    def forward(h):
        return pltpu.make_async_remote_copy(
            kv.at[h, :, TOK : 2 * TOK], kv.at[h, :, 3 * TOK : 4 * TOK], f_send.at[h], f_recv.at[h],
            device_id=partner, device_id_type=MESH,
        )

    def grads_to_partner(h):
        return pltpu.make_async_remote_copy(
            sd.at[h], rd.at[h], d_send.at[h], d_recv.at[h],
            device_id=partner, device_id_type=MESH,
        )

    def grads_across(h):
        return pltpu.make_async_remote_copy(
            si.at[h], ri.at[h], i_send.at[h], i_recv.at[h],
            device_id=across, device_id_type=MESH,
        )

    @pl.loop(0, KEY_VALUE_HEADS)
    def _(h):
        to_across(h).start()
        to_partner(h).start()

    first = lane < SPAN
    query_span = jnp.where(first, spans[0], spans[1])
    doc_row = jnp.zeros((8, TOK), F32)
    for part in range(LENGTH // TOK):
        row = seg_ref[pl.ds(seq * (LENGTH // TOK) + part, 1), :].astype(F32)
        segcol[part * TOK : (part + 1) * TOK, :] = jnp.transpose(
            jnp.broadcast_to(row, (TOK, TOK))
        )
        row = jnp.broadcast_to(row, (8, TOK))
        turned = pltpu.roll(row, SPAN, 1)
        doc_row = jnp.where(query_span == 2 * part, jnp.where(first, row, turned), doc_row)
        doc_row = jnp.where(query_span == 2 * part + 1, jnp.where(first, turned, row), doc_row)
    doc_row = doc_row[0:1, :]
    pos_row = (query_span * SPAN + jnp.bitwise_and(lane, SPAN - 1))[0:1, :]
    for index, span in enumerate(spans):
        doc_col = pick(span, segcol)
        pos_col = span[0:1, :] * SPAN + sub_iota
        allowed = (doc_col == doc_row) & (pos_col <= pos_row)
        bias[index * SPAN : (index + 1) * SPAN, :] = jnp.where(allowed, 0.0, -jnp.inf)

    @pl.loop(0, KEY_VALUE_HEADS)
    def _(h):
        for j in range(HEADS_PER):
            q_in(h, j).wait()
            g_in(h, j).wait()

    inner[...] = jnp.zeros((TOK, HEAD_SIZE), F32)

    @pl.loop(0, KEY_VALUE_HEADS)
    def _(h):
        total = inner[...]
        for j in range(HEADS_PER):
            x = q_vm[h, j * TOK : (j + 1) * TOK].astype(F32)
            total = total + x * x
        inner[...] = total

    mean_sq = jnp.sum(inner[...], axis=1, keepdims=True) * (1.0 / (QUERY_HEADS * HEAD_SIZE))
    rqb[...] = jnp.broadcast_to(lax.rsqrt(mean_sq + NORM_EPS), (TOK, HEAD_SIZE))
    inner[...] = jnp.zeros((TOK, HEAD_SIZE), F32)

    z_take = to_across(0)
    z_take.wait_recv()
    forward(0).start()

    def add_and_send(h):
        grads_to_partner(h).wait_recv()
        for s in range(2):
            si[h, s] = (mid[h, s] + rd[h, s, TOK : 2 * TOK]).astype(BF16)
        grads_across(h).start()

    CH = 64

    @pl.loop(0, KEY_VALUE_HEADS)
    def _(h):
        @pl.when(h < KEY_VALUE_HEADS - 1)
        def _():
            to_across(h + 1).wait_recv()
            forward(h + 1).start()

        for j in range(HEADS_PER):
            x = q_vm[h, j * TOK : (j + 1) * TOK].astype(F32)
            normed = x * rqb[...] * qg_ref[pl.ds(h * HEADS_PER + j, 1), :]
            qr[j * TOK : (j + 1) * TOK] = (
                normed * cosk[0:TOK] + swap_halves(normed) * sink[0:TOK]
            ).astype(BF16)

        to_partner(h).wait_recv()
        forward(h).wait_recv()
        nt = (((1,), (1,)), ((), ()))
        st[...] = lax.dot_general(kv[h, 0], qr[...], nt, preferred_element_type=F32)
        dp[...] = lax.dot_general(kv[h, 1], g_vm[h], nt, preferred_element_type=F32)

        for j in range(HEADS_PER):
            cols = slice(j * TOK, (j + 1) * TOK)
            top = jnp.full((8, TOK), -jnp.inf, F32)
            for c in range(LENGTH // CH):
                rows = slice(c * CH, (c + 1) * CH)
                s = st[rows, cols] * SCALE2 + bias[rows, :]
                st[rows, cols] = s
                top = jnp.maximum(top, jnp.max(s.reshape(CH // 8, 8, TOK), axis=0))
            top = jnp.max(top, axis=0, keepdims=True)
            weight = jnp.zeros((8, TOK), F32)
            delta = jnp.zeros((8, TOK), F32)
            for c in range(LENGTH // CH):
                rows = slice(c * CH, (c + 1) * CH)
                p = jnp.exp2(st[rows, cols] - top)
                st[rows, cols] = p
                weight = weight + jnp.sum(p.reshape(CH // 8, 8, TOK), axis=0)
                delta = delta + jnp.sum((p * dp[rows, cols]).reshape(CH // 8, 8, TOK), axis=0)
            norm = 1.0 / jnp.sum(weight, axis=0, keepdims=True)
            delta = jnp.sum(delta, axis=0, keepdims=True) * norm
            for c in range(LENGTH // CH):
                rows = slice(c * CH, (c + 1) * CH)
                p = st[rows, cols] * norm
                pt[rows, cols] = p.astype(BF16)
                ds[rows, cols] = (p * (dp[rows, cols] - delta)).astype(BF16)

        tn = (((0,), (0,)), ((), ()))
        dq = lax.dot_general(ds[...], kv[h, 0], tn, preferred_element_type=F32)
        for j in range(HEADS_PER):
            part = dq[j * TOK : (j + 1) * TOK] * SCALE
            part = part * cosk[0:TOK] - swap_halves(part) * sink[0:TOK]
            x = q_vm[h, j * TOK : (j + 1) * TOK].astype(F32)
            gpart[h, j : j + 1, :] = jnp.sum(part * x * rqb[...], axis=0, keepdims=True)
            weighted = part * qg_ref[pl.ds(h * HEADS_PER + j, 1), :]
            dqw[h, j * TOK : (j + 1) * TOK] = weighted
            inner[...] = inner[...] + weighted * x

        nn = (((1,), (0,)), ((), ()))
        dv = lax.dot_general(pt[...], g_vm[h], nn, preferred_element_type=F32)
        own[h, 1] = dv[0:TOK]
        mid[h, 1] = dv[TOK : 2 * TOK]
        sd[h, 1] = dv[2 * TOK :]
        dk = lax.dot_general(ds[...], qr[...], nn, preferred_element_type=F32) * SCALE
        own[h, 0] = dk[0:TOK]
        mid[h, 0] = dk[TOK : 2 * TOK]
        sd[h, 0] = dk[2 * TOK :]
        grads_to_partner(h).start()

        total = jnp.zeros((8, HEAD_SIZE), F32)
        for c in range(4):
            rows = slice(c * TOK, (c + 1) * TOK)
            d_part = dk[rows]
            k_part = kv[h, 0, rows].astype(F32)
            d_part = d_part * cosk[rows] - swap_halves(d_part) * sink[rows]
            k_part = k_part * cosk[rows] - swap_halves(k_part) * sink[rows]
            total = total + jnp.sum((d_part * k_part).reshape(TOK // 8, 8, HEAD_SIZE), axis=0)
        gpart[h, HEADS_PER : HEADS_PER + 1, :] = (
            jnp.sum(total, axis=0, keepdims=True) / kg_ref[pl.ds(h, 1), :]
        )
        gpart[h, HEADS_PER + 1 :, :] = jnp.zeros((7 - HEADS_PER, HEAD_SIZE), F32)

        @pl.when(h > 0)
        def _():
            add_and_send(h - 1)

    def shard_out(d):
        other = jnp.bitwise_xor(rank, d)
        return pltpu.make_async_remote_copy(
            gpart.at[other], rs.at[d], rs_send.at[d], rs_recv.at[d],
            device_id=rank_peer(other), device_id_type=MESH,
        )

    def z_out(d):
        return pltpu.make_async_remote_copy(
            zb.at[zi], zb.at[zi], zb_send.at[d], zb_recv.at[zi],
            device_id={"context_1": lax.rem(zi + d, nz)}, device_id_type=MESH,
        )

    def z_got(d):
        source = lax.rem(zi + d, nz)
        return pltpu.make_async_remote_copy(
            zb.at[source], zb.at[source], zb_send.at[d], zb_recv.at[source],
            device_id={"context_1": source}, device_id_type=MESH,
        )

    def total_out(d):
        other = jnp.bitwise_xor(rank, d)
        return pltpu.make_async_remote_copy(
            ag.at[rank], ag.at[rank], ag_send.at[d], ag_recv.at[rank],
            device_id=rank_peer(other), device_id_type=MESH,
        )

    def total_got(d):
        other = jnp.bitwise_xor(rank, d)
        return pltpu.make_async_remote_copy(
            ag.at[other], ag.at[other], ag_send.at[d], ag_recv.at[other],
            device_id=rank_peer(other), device_id_type=MESH,
        )

    for d in range(1, nx * nc):
        shard_out(d).start()

    add_and_send(KEY_VALUE_HEADS - 1)

    summed = gpart[rank]
    for d in range(1, nx * nc):
        shard_out(d).wait_recv()
        summed = summed + rs[d]
    zb[zi] = summed
    for d in range(1, nz):
        z_out(d).start()

    inner_q = jnp.sum(inner[...], axis=1, keepdims=True) * (1.0 / (QUERY_HEADS * HEAD_SIZE))
    cube = rqb[...] * rqb[...] * rqb[...] * inner_q
    inner[...] = cube

    def q_out(h, j):
        cols = pl.ds(pl.multiple_of((h * HEADS_PER + j) * HEAD_SIZE, HEAD_SIZE), HEAD_SIZE)
        rows = pl.ds(j * TOK, TOK)
        return pltpu.make_async_copy(outb.at[h, rows], qgrad_hbm.at[:, cols], out_sem.at[h, j])

    @pl.loop(0, KEY_VALUE_HEADS)
    def _(h):
        for j in range(HEADS_PER):
            rows = slice(j * TOK, (j + 1) * TOK)
            x = q_vm[h, rows].astype(F32)
            outb[h, rows] = (rqb[...] * dqw[h, rows] - x * inner[...]).astype(BF16)
            q_out(h, j).start()

    for d in range(1, nz):
        z_got(d).wait_recv()
    total = zb[0]
    for d in range(1, nz):
        total = total + zb[d]
    ag[rank] = total
    for d in range(1, nx * nc):
        total_out(d).start()

    def k_out(h, s, out):
        cols = pl.ds(pl.multiple_of(h * HEAD_SIZE, HEAD_SIZE), HEAD_SIZE)
        return pltpu.make_async_copy(si.at[h, s], out.at[:, cols], out_sem.at[h, HEADS_PER + s])

    inner[...] = jnp.zeros((TOK, HEAD_SIZE), F32)

    @pl.loop(0, KEY_VALUE_HEADS)
    def _(h):
        grads_across(h).wait()
        d_part = own[h, 0] + rd[h, 0, 0:TOK] + ri[h, 0].astype(F32)
        d_part = d_part * cosk[0:TOK] - swap_halves(d_part) * sink[0:TOK]
        weighted = d_part * kg_ref[pl.ds(h, 1), :]
        dkw[h] = weighted
        inner[...] = inner[...] + weighted * k_vm[h].astype(F32)
        si[h, 1] = (own[h, 1] + rd[h, 1, 0:TOK] + ri[h, 1].astype(F32)).astype(BF16)
        k_out(h, 1, vgrad_hbm).start()

    inner_k = jnp.sum(inner[...], axis=1, keepdims=True) * (1.0 / (KEY_VALUE_HEADS * HEAD_SIZE))
    inner[...] = rkb[...] * rkb[...] * rkb[...] * inner_k

    @pl.loop(0, KEY_VALUE_HEADS)
    def _(h):
        si[h, 0] = (rkb[...] * dkw[h] - k_vm[h].astype(F32) * inner[...]).astype(BF16)
        k_out(h, 0, kgrad_hbm).start()

    for d in range(1, nx * nc):
        total_got(d).wait_recv()
    for h in range(KEY_VALUE_HEADS):
        qgain_ref[h * HEADS_PER : (h + 1) * HEADS_PER, :] = ag[h, 0:HEADS_PER, :]
        kgain_ref[h : h + 1, :] = ag[h, HEADS_PER : HEADS_PER + 1, :]

    @pl.loop(0, KEY_VALUE_HEADS)
    def _(h):
        to_across(h).wait_send()
        to_partner(h).wait_send()
        forward(h).wait_send()
        grads_to_partner(h).wait_send()
        for j in range(HEADS_PER):
            q_out(h, j).wait()
        k_out(h, 0, kgrad_hbm).wait()
        k_out(h, 1, vgrad_hbm).wait()

    for d in range(1, nx * nc):
        shard_out(d).wait_send()
        total_out(d).wait_send()
    for d in range(1, nz):
        z_out(d).wait_send()


def body(nx, nz, nc, query_proj, key_proj, values, grad_out, query_gain, key_gain, segments, layout):
    cos_table, sin_table = rope_tables()
    assert nx * nc == KEY_VALUE_HEADS or nx * nc < KEY_VALUE_HEADS
    kvh, hs = KEY_VALUE_HEADS, HEAD_SIZE
    any_spec = pl.BlockSpec(memory_space=pl.ANY)
    vm_spec = pl.BlockSpec(memory_space=pltpu.VMEM)
    dma = pltpu.SemaphoreType.DMA
    out = pl.pallas_call(
        functools.partial(kernel, nx, nz, nc),
        out_shape=(
            jax.ShapeDtypeStruct(query_proj.shape, BF16),
            jax.ShapeDtypeStruct(key_proj.shape, BF16),
            jax.ShapeDtypeStruct(values.shape, BF16),
            jax.ShapeDtypeStruct((QUERY_HEADS, hs), F32),
            jax.ShapeDtypeStruct((kvh, hs), F32),
        ),
        in_specs=[any_spec] * 4 + [vm_spec] * 5 + [pl.BlockSpec(memory_space=pltpu.SMEM)],
        out_specs=(any_spec, any_spec, any_spec, vm_spec, vm_spec),
        scratch_shapes=[
            pltpu.VMEM((kvh, QROWS, hs), BF16),
            pltpu.VMEM((kvh, QROWS, hs), BF16),
            pltpu.VMEM((kvh, TOK, hs), BF16),
            pltpu.VMEM((kvh, 2, LENGTH, hs), BF16),
            pltpu.VMEM((QROWS, hs), BF16),
            pltpu.VMEM((LENGTH, QROWS), F32),
            pltpu.VMEM((LENGTH, QROWS), F32),
            pltpu.VMEM((LENGTH, QROWS), BF16),
            pltpu.VMEM((LENGTH, QROWS), BF16),
            pltpu.VMEM((kvh, QROWS, hs), F32),
            pltpu.VMEM((kvh, TOK, hs), F32),
            pltpu.VMEM((LENGTH, TOK), F32),
            pltpu.VMEM((LENGTH, TOK), F32),
            pltpu.VMEM((LENGTH, hs), F32),
            pltpu.VMEM((LENGTH, hs), F32),
            pltpu.VMEM((TOK, hs), F32),
            pltpu.VMEM((TOK, hs), F32),
            pltpu.VMEM((TOK, hs), F32),
            pltpu.VMEM((kvh, 2, TOK, hs), F32),
            pltpu.VMEM((kvh, 2, TOK, hs), F32),
            pltpu.VMEM((kvh, 2, 2 * TOK, hs), F32),
            pltpu.VMEM((kvh, 2, 2 * TOK, hs), F32),
            pltpu.VMEM((kvh, 2, TOK, hs), BF16),
            pltpu.VMEM((kvh, 2, TOK, hs), BF16),
            pltpu.VMEM((kvh, QROWS, hs), BF16),
            pltpu.VMEM((kvh, 8, hs), F32),
            pltpu.VMEM((nx * nc, 8, hs), F32),
            pltpu.VMEM((nz, 8, hs), F32),
            pltpu.VMEM((kvh, 8, hs), F32),
            dma((2, kvh, HEADS_PER)), dma((kvh,)), dma((kvh,)),
            dma((kvh,)), dma((kvh,)), dma((kvh,)), dma((kvh,)), dma((kvh,)), dma((kvh,)),
            dma((kvh,)), dma((kvh,)), dma((kvh,)), dma((kvh,)),
            dma((nx * nc,)), dma((nx * nc,)), dma((nz,)), dma((nz,)), dma((kvh,)), dma((kvh,)),
            dma((kvh, HEADS_PER + 2)),
        ],
        compiler_params=pltpu.CompilerParams(
            collective_id=0, has_side_effects=True, vmem_limit_bytes=56 * 1024 * 1024
        ),
    )(
        query_proj, key_proj, values, grad_out,
        query_gain.reshape(QUERY_HEADS, hs), key_gain.reshape(kvh, hs),
        segments.reshape(-1, TOK), jnp.asarray(cos_table), jnp.asarray(sin_table), layout,
    )
    return out[0], out[1], out[2], out[3].reshape(-1), out[4].reshape(-1)


def solution(mesh):
    nx, nz, nc = 4, 16, 2
    split = Mesh(mesh.devices.reshape(mesh.shape["groups"], nx, nz, nc), GROUPS_CONTEXT)
    tokens = P(GROUPS_CONTEXT, None)
    return jax.shard_map(
        functools.partial(body, nx, nz, nc),
        mesh=split,
        in_specs=(tokens, tokens, tokens, tokens, P(), P(), P("groups"), P("groups")),
        out_specs=(tokens, tokens, tokens, P("groups"), P("groups")),
        check_vma=False,
    )
```

```python
import functools
import math

import jax
import jax.numpy as jnp
import numpy as np
from jax import lax
from jax.experimental import pallas as pl
from jax.experimental.pallas import tpu as pltpu
from jax.sharding import Mesh
from jax.sharding import PartitionSpec as P

QUERY_HEADS = 40
KEY_VALUE_HEADS = 8
HEADS_PER = QUERY_HEADS // KEY_VALUE_HEADS
HEAD_SIZE = 128
SPAN = 64
LENGTH = 512
SPANS = LENGTH // SPAN
TOK = 128
QROWS = HEADS_PER * TOK
CONTEXT = ("context_0", "context_1", "context_2")
GROUPS_CONTEXT = ("groups", "context_0", "context_1", "context_2")
NORM_EPS = 1e-06
ROPE_BASE = 500000.0
SCALE = HEAD_SIZE ** (-0.5)
SCALE2 = SCALE * math.log2(math.e)
MESH = pl.DeviceIdType.MESH
F32 = jnp.float32
BF16 = jnp.bfloat16


def rope_tables():
    half = HEAD_SIZE // 2
    inv_freq = np.power(ROPE_BASE, -2.0 * np.arange(half) / HEAD_SIZE)
    angles = np.arange(LENGTH)[:, None] * inv_freq[None, :]
    cosine, sine = np.cos(angles), np.sin(angles)
    return (
        np.concatenate([cosine, cosine], axis=1).astype(np.float32),
        np.concatenate([-sine, sine], axis=1).astype(np.float32),
    )


def swap_halves(x):
    return pltpu.roll(x, HEAD_SIZE // 2, 1)


def kernel(
    nx, nz, nc,
    q_hbm, k_hbm, v_hbm, g_hbm, cos_hbm, sin_hbm, seg_hbm, qg_ref, kg_ref, lay_ref,
    qgrad_hbm, kgrad_hbm, vgrad_hbm, qgain_ref, kgain_ref,
    cos_ref, sin_ref, seg_ref,
    q_vm, g_vm, k_vm, kv, qr, st, dp, pt, ds, dqw, dkw,
    bias, segcol, cosk, sink, cq, sq, rqb, rkb, inner,
    own, mid, sd, rd, si, ri, outb,
    gpart, rs, zb, ag,
    in_sem, kin_sem, vin_sem, tab_sem,
    z_send, z_recv, c_send, c_recv, f_send, f_recv,
    d_send, d_recv, i_send, i_recv,
    rs_send, rs_recv, zb_send, zb_recv, ag_send, ag_recv, out_sem,
):
    xi = lax.axis_index("context_0")
    zi = lax.axis_index("context_1")
    ci = lax.axis_index("context_2")
    rank = xi * nc + ci
    seq = xi * (nz // 2) + zi // 2
    z_flip = zi + 1 - 2 * lax.rem(zi, 2)
    partner = {"context_2": 1 - ci}
    across = {"context_1": z_flip}

    def rank_peer(other):
        return {"context_0": other // nc, "context_2": lax.rem(other, nc)}

    def k_in(h):
        cols = pl.ds(pl.multiple_of(h * HEAD_SIZE, HEAD_SIZE), HEAD_SIZE)
        return pltpu.make_async_copy(k_hbm.at[:, cols], k_vm.at[h], kin_sem.at[h])

    def v_in(h):
        cols = pl.ds(pl.multiple_of(h * HEAD_SIZE, HEAD_SIZE), HEAD_SIZE)
        return pltpu.make_async_copy(v_hbm.at[:, cols], kv.at[h, 1, 0:TOK], vin_sem.at[h])

    def q_in(h, j):
        cols = pl.ds(pl.multiple_of((h * HEADS_PER + j) * HEAD_SIZE, HEAD_SIZE), HEAD_SIZE)
        rows = pl.ds(j * TOK, TOK)
        return pltpu.make_async_copy(q_hbm.at[:, cols], q_vm.at[h, rows], in_sem.at[0, h, j])

    def g_in(h, j):
        cols = pl.ds(pl.multiple_of((h * HEADS_PER + j) * HEAD_SIZE, HEAD_SIZE), HEAD_SIZE)
        rows = pl.ds(j * TOK, TOK)
        return pltpu.make_async_copy(g_hbm.at[:, cols], g_vm.at[h, rows], in_sem.at[1, h, j])

    tables = [
        pltpu.make_async_copy(source, target, tab_sem.at[index])
        for index, (source, target) in enumerate(
            ((cos_hbm, cos_ref), (sin_hbm, sin_ref), (seg_hbm, seg_ref))
        )
    ]
    for h in range(KEY_VALUE_HEADS):
        v_in(h).start()
        k_in(h).start()
    for table in tables:
        table.start()

    barrier = pltpu.get_barrier_semaphore()
    for d in range(1, nx * nc):
        pl.semaphore_signal(
            barrier, inc=1, device_id=rank_peer(jnp.bitwise_xor(rank, d)), device_id_type=MESH
        )
    for d in range(1, nz):
        pl.semaphore_signal(
            barrier, inc=1, device_id={"context_1": lax.rem(zi + d, nz)}, device_id_type=MESH
        )

    my_local = 2 * lax.rem(zi, 2) + ci
    sub_iota = lax.broadcasted_iota(jnp.int32, (SPAN, TOK), 0)
    lane = lax.broadcasted_iota(jnp.int32, (8, TOK), 1)
    spans = []
    for flip in (0, 2, 1, 3):
        holder = jnp.bitwise_xor(my_local, flip)
        for part in range(2):
            slot = lay_ref[seq * SPANS + 2 * holder + part]
            spans.append(jnp.bitwise_and(jnp.full((8, TOK), slot, jnp.int32), SPANS - 1))

    def pick(span, table):
        chosen = table[0:SPAN, :]
        wide = jnp.concatenate([span] * (SPAN // 8), axis=0)
        for at in range(1, SPANS):
            chosen = jnp.where(wide == at, table[at * SPAN : (at + 1) * SPAN, :], chosen)
        return chosen

    def key_rotary(index):
        rows = slice(index * SPAN, (index + 1) * SPAN)
        cosk[rows, :] = pick(spans[index], cos_ref)
        sink[rows, :] = pick(spans[index], sin_ref)

    def to_across(s, h):
        return pltpu.make_async_remote_copy(
            kv.at[h, s, 0:TOK], kv.at[h, s, TOK : 2 * TOK], z_send.at[s, h], z_recv.at[s, h],
            device_id=across, device_id_type=MESH,
        )

    def to_partner(s, h):
        return pltpu.make_async_remote_copy(
            kv.at[h, s, 0:TOK], kv.at[h, s, 2 * TOK : 3 * TOK], c_send.at[s, h], c_recv.at[s, h],
            device_id=partner, device_id_type=MESH,
        )

    def forward(h):
        return pltpu.make_async_remote_copy(
            kv.at[h, :, TOK : 2 * TOK], kv.at[h, :, 3 * TOK : 4 * TOK], f_send.at[h], f_recv.at[h],
            device_id=partner, device_id_type=MESH,
        )

    def grads_to_partner(h):
        return pltpu.make_async_remote_copy(
            sd.at[h], rd.at[h], d_send.at[h], d_recv.at[h],
            device_id=partner, device_id_type=MESH,
        )

    def grads_across(h):
        return pltpu.make_async_remote_copy(
            si.at[h], ri.at[h], i_send.at[h], i_recv.at[h],
            device_id=across, device_id_type=MESH,
        )

    def values_out(h):
        v_in(h).wait()
        to_across(1, h).start()
        to_partner(1, h).start()

    AHEAD = 2
    pl.semaphore_wait(barrier, nx * nc - 1 + nz - 1)
    for h in range(AHEAD):
        values_out(h)

    @pl.loop(0, KEY_VALUE_HEADS)
    def _(h):
        for j in range(HEADS_PER):
            q_in(h, j).start()
            g_in(h, j).start()

    for h in range(KEY_VALUE_HEADS):
        k_in(h).wait()
    acc = jnp.zeros((TOK, HEAD_SIZE), F32)
    for h in range(KEY_VALUE_HEADS):
        x = k_vm[h].astype(F32)
        acc = acc + x * x
    mean_sq = jnp.sum(acc, axis=1, keepdims=True) * (1.0 / (KEY_VALUE_HEADS * HEAD_SIZE))
    rkb[...] = jnp.broadcast_to(lax.rsqrt(mean_sq + NORM_EPS), (TOK, HEAD_SIZE))
    for table in tables:
        table.wait()
    key_rotary(0)
    key_rotary(1)

    @pl.loop(0, KEY_VALUE_HEADS)
    def _(h):
        normed = k_vm[h].astype(F32) * rkb[...] * kg_ref[pl.ds(h, 1), :]
        kv[h, 0, 0:TOK] = (normed * cosk[0:TOK] + swap_halves(normed) * sink[0:TOK]).astype(BF16)
        to_across(0, h).start()
        to_partner(0, h).start()

        @pl.when(h < KEY_VALUE_HEADS - AHEAD)
        def _():
            values_out(h + AHEAD)

    cq[...] = cosk[0:TOK] * SCALE
    sq[...] = sink[0:TOK] * SCALE
    for index in range(2, SPANS):
        key_rotary(index)

    first = lane < SPAN
    query_span = jnp.where(first, spans[0], spans[1])
    doc_row = jnp.zeros((8, TOK), F32)
    for part in range(LENGTH // TOK):
        row = seg_ref[pl.ds(seq * (LENGTH // TOK) + part, 1), :].astype(F32)
        segcol[part * TOK : (part + 1) * TOK, :] = jnp.transpose(
            jnp.broadcast_to(row, (TOK, TOK))
        )
        row = jnp.broadcast_to(row, (8, TOK))
        turned = pltpu.roll(row, SPAN, 1)
        doc_row = jnp.where(query_span == 2 * part, jnp.where(first, row, turned), doc_row)
        doc_row = jnp.where(query_span == 2 * part + 1, jnp.where(first, turned, row), doc_row)
    doc_row = doc_row[0:1, :]
    pos_row = (query_span * SPAN + jnp.bitwise_and(lane, SPAN - 1))[0:1, :]
    for index, span in enumerate(spans):
        doc_col = pick(span, segcol)
        pos_col = span[0:1, :] * SPAN + sub_iota
        allowed = (doc_col == doc_row) & (pos_col <= pos_row)
        bias[index * SPAN : (index + 1) * SPAN, :] = jnp.where(allowed, 0.0, -jnp.inf)

    @pl.loop(0, KEY_VALUE_HEADS)
    def _(h):
        for j in range(HEADS_PER):
            q_in(h, j).wait()
            g_in(h, j).wait()

    inner[...] = jnp.zeros((TOK, HEAD_SIZE), F32)

    @pl.loop(0, KEY_VALUE_HEADS)
    def _(h):
        total = inner[...]
        for j in range(HEADS_PER):
            x = q_vm[h, j * TOK : (j + 1) * TOK].astype(F32)
            total = total + x * x
        inner[...] = total

    mean_sq = jnp.sum(inner[...], axis=1, keepdims=True) * (1.0 / (QUERY_HEADS * HEAD_SIZE))
    rqb[...] = jnp.broadcast_to(lax.rsqrt(mean_sq + NORM_EPS), (TOK, HEAD_SIZE))
    inner[...] = jnp.zeros((TOK, HEAD_SIZE), F32)

    def take(h):
        to_across(0, h).wait_recv()
        to_across(1, h).wait_recv()
        forward(h).start()

    @pl.loop(0, KEY_VALUE_HEADS)
    def _(h):
        for j in range(HEADS_PER):
            rows = slice(j * TOK, (j + 1) * TOK)
            normed = q_vm[h, rows].astype(F32) * rqb[...] * qg_ref[pl.ds(h * HEADS_PER + j, 1), :]
            qr[h, rows] = (
                normed * cosk[0:TOK] + swap_halves(normed) * sink[0:TOK]
            ).astype(BF16)

    take(0)

    def add_and_send(h):
        grads_to_partner(h).wait_recv()
        for s in range(2):
            si[h, s] = (mid[h, s] + rd[h, s, TOK : 2 * TOK]).astype(BF16)
        grads_across(h).start()

    CH = 64

    @pl.loop(0, KEY_VALUE_HEADS)
    def _(h):
        @pl.when(h < KEY_VALUE_HEADS - 1)
        def _():
            take(h + 1)

        to_partner(0, h).wait_recv()
        to_partner(1, h).wait_recv()
        forward(h).wait_recv()
        nt = (((1,), (1,)), ((), ()))
        tn = (((0,), (0,)), ((), ()))
        nn = (((1,), (0,)), ((), ()))

        def scores(lo, hi):
            part = slice(lo * TOK, hi * TOK)
            raw = lax.dot_general(kv[h, 0], qr[h, part], nt, preferred_element_type=F32)
            st[:, part] = raw
            tops = []
            for j in range(hi - lo):
                cols = slice(j * TOK, (j + 1) * TOK)
                top = jnp.full((8, TOK), -jnp.inf, F32)
                for c in range(LENGTH // CH):
                    rows = slice(c * CH, (c + 1) * CH)
                    masked = raw[rows, cols] + bias[rows, :]
                    top = jnp.maximum(top, jnp.max(masked.reshape(CH // 8, 8, TOK), axis=0))
                tops.append(jnp.max(top, axis=0, keepdims=True) * SCALE2)
            dp[:, part] = lax.dot_general(kv[h, 1], g_vm[h, part], nt, preferred_element_type=F32)
            return tops

        def softmax(j, top):
            cols = slice(j * TOK, (j + 1) * TOK)
            weight = jnp.zeros((8, TOK), F32)
            delta = jnp.zeros((8, TOK), F32)
            for c in range(LENGTH // CH):
                rows = slice(c * CH, (c + 1) * CH)
                p = jnp.exp2((st[rows, cols] + bias[rows, :]) * SCALE2 - top)
                st[rows, cols] = p
                weight = weight + jnp.sum(p.reshape(CH // 8, 8, TOK), axis=0)
                delta = delta + jnp.sum((p * dp[rows, cols]).reshape(CH // 8, 8, TOK), axis=0)
            norm = 1.0 / jnp.sum(weight, axis=0, keepdims=True)
            delta = jnp.sum(delta, axis=0, keepdims=True) * norm
            for c in range(LENGTH // CH):
                rows = slice(c * CH, (c + 1) * CH)
                p = st[rows, cols] * norm
                pt[rows, cols] = p.astype(BF16)
                ds[rows, cols] = (p * (dp[rows, cols] - delta)).astype(BF16)

        def query_grads(lo, hi):
            part = slice(lo * TOK, hi * TOK)
            dq = lax.dot_general(ds[:, part], kv[h, 0], tn, preferred_element_type=F32)
            along = jnp.zeros((TOK, HEAD_SIZE), F32)
            for j in range(lo, hi):
                d_part = dq[(j - lo) * TOK : (j - lo + 1) * TOK]
                d_part = d_part * cq[...] - swap_halves(d_part) * sq[...]
                dqw[h, j * TOK : (j + 1) * TOK] = d_part
                d_part = d_part * q_vm[h, j * TOK : (j + 1) * TOK].astype(F32)
                gpart[h, j : j + 1, :] = jnp.sum(d_part * rqb[...], axis=0, keepdims=True)
                along = along + d_part * qg_ref[pl.ds(h * HEADS_PER + j, 1), :]
            inner[...] = inner[...] + along

        def key_grads(lo, hi):
            part = slice(lo * TOK, hi * TOK)
            dv = lax.dot_general(pt[:, part], g_vm[h, part], nn, preferred_element_type=F32)
            dk = lax.dot_general(ds[:, part], qr[h, part], nn, preferred_element_type=F32)
            return dk, dv

        tops = scores(0, 2) + scores(2, 4) + scores(4, 5)
        for j in range(HEADS_PER):
            softmax(j, tops[j])
        query_grads(0, HEADS_PER)
        dk, dv = key_grads(0, HEADS_PER)
        own[h, 1] = dv[0:TOK]
        mid[h, 1] = dv[TOK : 2 * TOK]
        sd[h, 1] = dv[2 * TOK :]
        own[h, 0] = dk[0:TOK]
        mid[h, 0] = dk[TOK : 2 * TOK]
        sd[h, 0] = dk[2 * TOK :]
        grads_to_partner(h).start()

        total = jnp.zeros((8, HEAD_SIZE), F32)
        for c in range(4):
            rows = slice(c * TOK, (c + 1) * TOK)
            d_part = dk[rows]
            k_part = kv[h, 0, rows].astype(F32)
            d_part = d_part * cosk[rows] - swap_halves(d_part) * sink[rows]
            k_part = k_part * cosk[rows] - swap_halves(k_part) * sink[rows]
            total = total + jnp.sum((d_part * k_part).reshape(TOK // 8, 8, HEAD_SIZE), axis=0)
        gpart[h, HEADS_PER : HEADS_PER + 1, :] = (
            jnp.sum(total, axis=0, keepdims=True) * SCALE / kg_ref[pl.ds(h, 1), :]
        )
        gpart[h, HEADS_PER + 1 :, :] = jnp.zeros((7 - HEADS_PER, HEAD_SIZE), F32)

        @pl.when(h > 0)
        def _():
            add_and_send(h - 1)

    def shard_out(d):
        other = jnp.bitwise_xor(rank, d)
        return pltpu.make_async_remote_copy(
            gpart.at[other], rs.at[d], rs_send.at[d], rs_recv.at[d],
            device_id=rank_peer(other), device_id_type=MESH,
        )

    def z_out(d):
        return pltpu.make_async_remote_copy(
            zb.at[zi], zb.at[zi], zb_send.at[d], zb_recv.at[zi],
            device_id={"context_1": lax.rem(zi + d, nz)}, device_id_type=MESH,
        )

    def z_got(d):
        source = lax.rem(zi + d, nz)
        return pltpu.make_async_remote_copy(
            zb.at[source], zb.at[source], zb_send.at[d], zb_recv.at[source],
            device_id={"context_1": source}, device_id_type=MESH,
        )

    def total_out(d):
        other = jnp.bitwise_xor(rank, d)
        return pltpu.make_async_remote_copy(
            ag.at[rank], ag.at[rank], ag_send.at[d], ag_recv.at[rank],
            device_id=rank_peer(other), device_id_type=MESH,
        )

    def total_got(d):
        other = jnp.bitwise_xor(rank, d)
        return pltpu.make_async_remote_copy(
            ag.at[other], ag.at[other], ag_send.at[d], ag_recv.at[other],
            device_id=rank_peer(other), device_id_type=MESH,
        )

    for d in range(1, nx * nc):
        shard_out(d).start()

    add_and_send(KEY_VALUE_HEADS - 1)

    summed = gpart[rank]
    for d in range(1, nx * nc):
        shard_out(d).wait_recv()
        summed = summed + rs[d]
    zb[zi] = summed
    for d in range(1, nz):
        z_out(d).start()

    inner_q = jnp.sum(inner[...], axis=1, keepdims=True) * (1.0 / (QUERY_HEADS * HEAD_SIZE))
    cube = rqb[...] * rqb[...] * rqb[...] * inner_q
    inner[...] = cube

    def q_out(h, j):
        cols = pl.ds(pl.multiple_of((h * HEADS_PER + j) * HEAD_SIZE, HEAD_SIZE), HEAD_SIZE)
        rows = pl.ds(j * TOK, TOK)
        return pltpu.make_async_copy(outb.at[h, rows], qgrad_hbm.at[:, cols], out_sem.at[h, j])

    @pl.loop(0, KEY_VALUE_HEADS)
    def _(h):
        for j in range(HEADS_PER):
            rows = slice(j * TOK, (j + 1) * TOK)
            x = q_vm[h, rows].astype(F32)
            weighted = dqw[h, rows] * qg_ref[pl.ds(h * HEADS_PER + j, 1), :]
            outb[h, rows] = (rqb[...] * weighted - x * inner[...]).astype(BF16)
            q_out(h, j).start()

    for d in range(1, nz):
        z_got(d).wait_recv()
    total = zb[0]
    for d in range(1, nz):
        total = total + zb[d]
    ag[rank] = total
    for d in range(1, nx * nc):
        total_out(d).start()

    def k_out(h, s, out):
        cols = pl.ds(pl.multiple_of(h * HEAD_SIZE, HEAD_SIZE), HEAD_SIZE)
        return pltpu.make_async_copy(si.at[h, s], out.at[:, cols], out_sem.at[h, HEADS_PER + s])

    inner[...] = jnp.zeros((TOK, HEAD_SIZE), F32)

    @pl.loop(0, KEY_VALUE_HEADS)
    def _(h):
        grads_across(h).wait()
        d_part = own[h, 0] + rd[h, 0, 0:TOK] + ri[h, 0].astype(F32)
        d_part = d_part * cq[...] - swap_halves(d_part) * sq[...]
        weighted = d_part * kg_ref[pl.ds(h, 1), :]
        dkw[h] = weighted
        inner[...] = inner[...] + weighted * k_vm[h].astype(F32)
        si[h, 1] = (own[h, 1] + rd[h, 1, 0:TOK] + ri[h, 1].astype(F32)).astype(BF16)
        k_out(h, 1, vgrad_hbm).start()

    inner_k = jnp.sum(inner[...], axis=1, keepdims=True) * (1.0 / (KEY_VALUE_HEADS * HEAD_SIZE))
    inner[...] = rkb[...] * rkb[...] * rkb[...] * inner_k

    @pl.loop(0, KEY_VALUE_HEADS)
    def _(h):
        si[h, 0] = (rkb[...] * dkw[h] - k_vm[h].astype(F32) * inner[...]).astype(BF16)
        k_out(h, 0, kgrad_hbm).start()

    for d in range(1, nx * nc):
        total_got(d).wait_recv()
    for h in range(KEY_VALUE_HEADS):
        qgain_ref[h * HEADS_PER : (h + 1) * HEADS_PER, :] = ag[h, 0:HEADS_PER, :]
        kgain_ref[h : h + 1, :] = ag[h, HEADS_PER : HEADS_PER + 1, :]

    @pl.loop(0, KEY_VALUE_HEADS)
    def _(h):
        for s in range(2):
            to_across(s, h).wait_send()
            to_partner(s, h).wait_send()
        forward(h).wait_send()
        grads_to_partner(h).wait_send()
        for j in range(HEADS_PER):
            q_out(h, j).wait()
        k_out(h, 0, kgrad_hbm).wait()
        k_out(h, 1, vgrad_hbm).wait()

    for d in range(1, nx * nc):
        shard_out(d).wait_send()
        total_out(d).wait_send()
    for d in range(1, nz):
        z_out(d).wait_send()


def settle(*refs):
    copies = [
        pltpu.make_async_copy(refs[i], refs[5 + i], refs[10].at[i]) for i in range(5)
    ]
    for copy in copies:
        copy.start()
    for copy in copies:
        copy.wait()


def body(nx, nz, nc, query_proj, key_proj, values, grad_out, query_gain, key_gain, segments, layout):
    cos_table, sin_table = rope_tables()
    assert nx * nc == KEY_VALUE_HEADS or nx * nc < KEY_VALUE_HEADS
    kvh, hs = KEY_VALUE_HEADS, HEAD_SIZE
    any_spec = pl.BlockSpec(memory_space=pl.ANY)
    vm_spec = pl.BlockSpec(memory_space=pltpu.VMEM)
    dma = pltpu.SemaphoreType.DMA
    out = pl.pallas_call(
        functools.partial(kernel, nx, nz, nc),
        out_shape=(
            jax.ShapeDtypeStruct(query_proj.shape, BF16),
            jax.ShapeDtypeStruct(key_proj.shape, BF16),
            jax.ShapeDtypeStruct(values.shape, BF16),
            jax.ShapeDtypeStruct((QUERY_HEADS, hs), F32),
            jax.ShapeDtypeStruct((kvh, hs), F32),
        ),
        in_specs=[pl.BlockSpec(memory_space=pltpu.HBM)] * 7 + [vm_spec] * 2 + [pl.BlockSpec(memory_space=pltpu.SMEM)],
        out_specs=(any_spec, any_spec, any_spec, vm_spec, vm_spec),
        scratch_shapes=[
            pltpu.VMEM((LENGTH, hs), F32),
            pltpu.VMEM((LENGTH, hs), F32),
            pltpu.VMEM((segments.shape[0] // TOK, TOK), jnp.int32),
            pltpu.VMEM((kvh, QROWS, hs), BF16),
            pltpu.VMEM((kvh, QROWS, hs), BF16),
            pltpu.VMEM((kvh, TOK, hs), BF16),
            pltpu.VMEM((kvh, 2, LENGTH, hs), BF16),
            pltpu.VMEM((kvh, QROWS, hs), BF16),
            pltpu.VMEM((LENGTH, QROWS), F32),
            pltpu.VMEM((LENGTH, QROWS), F32),
            pltpu.VMEM((LENGTH, QROWS), BF16),
            pltpu.VMEM((LENGTH, QROWS), BF16),
            pltpu.VMEM((kvh, QROWS, hs), F32),
            pltpu.VMEM((kvh, TOK, hs), F32),
            pltpu.VMEM((LENGTH, TOK), F32),
            pltpu.VMEM((LENGTH, TOK), F32),
            pltpu.VMEM((LENGTH, hs), F32),
            pltpu.VMEM((LENGTH, hs), F32),
            pltpu.VMEM((TOK, hs), F32),
            pltpu.VMEM((TOK, hs), F32),
            pltpu.VMEM((TOK, hs), F32),
            pltpu.VMEM((TOK, hs), F32),
            pltpu.VMEM((TOK, hs), F32),
            pltpu.VMEM((kvh, 2, TOK, hs), F32),
            pltpu.VMEM((kvh, 2, TOK, hs), F32),
            pltpu.VMEM((kvh, 2, 2 * TOK, hs), F32),
            pltpu.VMEM((kvh, 2, 2 * TOK, hs), F32),
            pltpu.VMEM((kvh, 2, TOK, hs), BF16),
            pltpu.VMEM((kvh, 2, TOK, hs), BF16),
            pltpu.VMEM((kvh, QROWS, hs), BF16),
            pltpu.VMEM((kvh, 8, hs), F32),
            pltpu.VMEM((nx * nc, 8, hs), F32),
            pltpu.VMEM((nz, 8, hs), F32),
            pltpu.VMEM((kvh, 8, hs), F32),
            dma((2, kvh, HEADS_PER)), dma((kvh,)), dma((kvh,)), dma((3,)),
            dma((2, kvh)), dma((2, kvh)), dma((2, kvh)), dma((2, kvh)), dma((kvh,)), dma((kvh,)),
            dma((kvh,)), dma((kvh,)), dma((kvh,)), dma((kvh,)),
            dma((nx * nc,)), dma((nx * nc,)), dma((nz,)), dma((nz,)), dma((kvh,)), dma((kvh,)),
            dma((kvh, HEADS_PER + 2)),
        ],
        compiler_params=pltpu.CompilerParams(
            collective_id=0, has_side_effects=True, vmem_limit_bytes=36 * 1024 * 1024
        ),
    )(
        *(
            pltpu.with_memory_space_constraint(x, pltpu.HBM)
            for x in (
                query_proj, key_proj, values, grad_out,
                jnp.asarray(cos_table), jnp.asarray(sin_table), segments.reshape(-1, TOK),
                query_gain.reshape(QUERY_HEADS, hs), key_gain.reshape(kvh, hs), layout,
            )
        ),
    )
    out = pl.pallas_call(
        settle,
        out_shape=[jax.ShapeDtypeStruct(o.shape, o.dtype) for o in out],
        in_specs=[any_spec] * 5,
        out_specs=[any_spec] * 5,
        scratch_shapes=[dma((5,))],
        compiler_params=pltpu.CompilerParams(vmem_limit_bytes=1024 * 1024),
    )(*out)
    return out[0], out[1], out[2], out[3].reshape(-1), out[4].reshape(-1)


def solution(mesh):
    nx, nz, nc = 4, 16, 2
    split = Mesh(mesh.devices.reshape(mesh.shape["groups"], nx, nz, nc), GROUPS_CONTEXT)
    tokens = P(GROUPS_CONTEXT, None)
    return jax.shard_map(
        functools.partial(body, nx, nz, nc),
        mesh=split,
        in_specs=(tokens, tokens, tokens, tokens, P(), P(), P("groups"), P("groups")),
        out_specs=(tokens, tokens, tokens, P("groups"), P("groups")),
        check_vma=False,
    )
```

```python
import functools
import math

import jax
import jax.numpy as jnp
import numpy as np
from jax import lax
from jax.experimental import pallas as pl
from jax.experimental.pallas import tpu as pltpu
from jax.sharding import Mesh
from jax.sharding import PartitionSpec as P

QUERY_HEADS = 40
KEY_VALUE_HEADS = 8
HEADS_PER = QUERY_HEADS // KEY_VALUE_HEADS
HEAD_SIZE = 128
SPAN = 64
LENGTH = 512
SPANS = LENGTH // SPAN
TOK = 128
QROWS = HEADS_PER * TOK
CONTEXT = ("context_0", "context_1", "context_2")
GROUPS_CONTEXT = ("groups", "context_0", "context_1", "context_2")
LATE = 2
EARLY = KEY_VALUE_HEADS - LATE
NORM_EPS = 1e-06
ROPE_BASE = 500000.0
SCALE = HEAD_SIZE ** (-0.5)
SCALE2 = SCALE * math.log2(math.e)
MESH = pl.DeviceIdType.MESH
F32 = jnp.float32
BF16 = jnp.bfloat16


def rope_tables():
    half = HEAD_SIZE // 2
    inv_freq = np.power(ROPE_BASE, -2.0 * np.arange(half) / HEAD_SIZE)
    angles = np.arange(LENGTH)[:, None] * inv_freq[None, :]
    cosine, sine = np.cos(angles), np.sin(angles)
    return (
        np.concatenate([cosine, cosine], axis=1).astype(np.float32),
        np.concatenate([-sine, sine], axis=1).astype(np.float32),
    )


def swap_halves(x):
    return pltpu.roll(x, HEAD_SIZE // 2, 1)


def kernel(
    nx, nz, nc,
    q_hbm, k_hbm, v_hbm, g_hbm, cos_hbm, sin_hbm, seg_hbm, qg_ref, kg_ref, lay_ref,
    qgrad_hbm, kgrad_hbm, vgrad_hbm, qgain_ref, kgain_ref,
    cos_ref, sin_ref, seg_ref,
    q_vm, g_vm, k_vm, kv, qr, st0, st1, dp0, dp1, pt, ds, dqw, dkw,
    bias, segcol, cosk, sink, cq, sq, rqb, rkb, inner,
    own, mid, sd, rd, si, ri, outb,
    tops0, tops1, gpart, rs, pf, za, zf, ag,
    in_sem, kin_sem, vin_sem, tab_sem,
    z_send, z_recv, c_send, c_recv, f_send, f_recv,
    d_send, d_recv, i_send, i_recv,
    rs_send, rs_recv, pf_send, pf_recv, za_send, za_recv, zf_send, zf_recv, ag_send, ag_recv,
    out_sem,
):
    xi = lax.axis_index("context_0")
    zi = lax.axis_index("context_1")
    ci = lax.axis_index("context_2")
    rank = xi * nc + ci
    seq = xi * (nz // 2) + zi // 2
    z_flip = zi + 1 - 2 * lax.rem(zi, 2)
    partner = {"context_2": 1 - ci}
    across = {"context_1": z_flip}

    def rank_peer(other):
        return {"context_0": other // nc, "context_2": lax.rem(other, nc)}

    def k_in(h):
        cols = pl.ds(pl.multiple_of(h * HEAD_SIZE, HEAD_SIZE), HEAD_SIZE)
        return pltpu.make_async_copy(k_hbm.at[:, cols], k_vm.at[h], kin_sem.at[0])

    def v_in(h):
        cols = pl.ds(pl.multiple_of(h * HEAD_SIZE, HEAD_SIZE), HEAD_SIZE)
        return pltpu.make_async_copy(v_hbm.at[:, cols], kv.at[h, 1, 0:TOK], vin_sem.at[h])

    def q_in(h, j):
        cols = pl.ds(pl.multiple_of((h * HEADS_PER + j) * HEAD_SIZE, HEAD_SIZE), HEAD_SIZE)
        rows = pl.ds(j * TOK, TOK)
        return pltpu.make_async_copy(q_hbm.at[:, cols], q_vm.at[h, rows], kin_sem.at[1])

    def g_in(h, j):
        cols = pl.ds(pl.multiple_of((h * HEADS_PER + j) * HEAD_SIZE, HEAD_SIZE), HEAD_SIZE)
        rows = pl.ds(j * TOK, TOK)
        return pltpu.make_async_copy(g_hbm.at[:, cols], g_vm.at[h, rows], in_sem.at[h])

    tables = [
        pltpu.make_async_copy(source, target, tab_sem.at[index])
        for index, (source, target) in enumerate(
            ((cos_hbm, cos_ref), (sin_hbm, sin_ref), (seg_hbm, seg_ref))
        )
    ]
    for h in range(KEY_VALUE_HEADS):
        v_in(h).start()
        k_in(h).start()
    for table in tables:
        table.start()

    barrier = pltpu.get_barrier_semaphore()
    for d in range(1, nx * nc):
        pl.semaphore_signal(
            barrier, inc=1, device_id=rank_peer(jnp.bitwise_xor(rank, d)), device_id_type=MESH
        )
    for d in range(1, nz):
        pl.semaphore_signal(
            barrier, inc=1, device_id={"context_1": lax.rem(zi + d, nz)}, device_id_type=MESH
        )

    my_local = 2 * lax.rem(zi, 2) + ci
    sub_iota = lax.broadcasted_iota(jnp.int32, (SPAN, TOK), 0)
    lane = lax.broadcasted_iota(jnp.int32, (8, TOK), 1)
    spans = []
    for flip in (0, 2, 1, 3):
        holder = jnp.bitwise_xor(my_local, flip)
        for part in range(2):
            slot = lay_ref[seq * SPANS + 2 * holder + part]
            spans.append(jnp.bitwise_and(jnp.full((8, TOK), slot, jnp.int32), SPANS - 1))

    def pick(span, table):
        chosen = table[0:SPAN, :]
        wide = jnp.concatenate([span] * (SPAN // 8), axis=0)
        for at in range(1, SPANS):
            chosen = jnp.where(wide == at, table[at * SPAN : (at + 1) * SPAN, :], chosen)
        return chosen

    def key_rotary(index):
        rows = slice(index * SPAN, (index + 1) * SPAN)
        cosk[rows, :] = pick(spans[index], cos_ref)
        sink[rows, :] = pick(spans[index], sin_ref)

    def to_across(s, h):
        return pltpu.make_async_remote_copy(
            kv.at[h, s, 0:TOK], kv.at[h, s, TOK : 2 * TOK], z_send.at[s, h], z_recv.at[s, h],
            device_id=across, device_id_type=MESH,
        )

    def to_partner(s, h):
        return pltpu.make_async_remote_copy(
            kv.at[h, s, 0:TOK], kv.at[h, s, 2 * TOK : 3 * TOK], c_send.at[s, h], c_recv.at[s, h],
            device_id=partner, device_id_type=MESH,
        )

    def forward(h):
        return pltpu.make_async_remote_copy(
            kv.at[h, :, TOK : 2 * TOK], kv.at[h, :, 3 * TOK : 4 * TOK], f_send.at[h], f_recv.at[h],
            device_id=partner, device_id_type=MESH,
        )

    def grads_to_partner(h):
        return pltpu.make_async_remote_copy(
            sd.at[h], rd.at[h], d_send.at[h], d_recv.at[h],
            device_id=partner, device_id_type=MESH,
        )

    def grads_across(h):
        return pltpu.make_async_remote_copy(
            si.at[h], ri.at[h], i_send.at[h], i_recv.at[h],
            device_id=across, device_id_type=MESH,
        )

    def values_out(h):
        v_in(h).wait()
        to_across(1, h).start()
        to_partner(1, h).start()

    AHEAD = 2
    pl.semaphore_wait(barrier, nx * nc - 1 + nz - 1)
    for h in range(AHEAD):
        values_out(h)

    @pl.loop(0, KEY_VALUE_HEADS)
    def _(h):
        for j in range(HEADS_PER):
            q_in(h, j).start()
            g_in(h, j).start()

    pltpu.make_async_copy(k_vm, k_vm, kin_sem.at[0]).wait()
    acc = jnp.zeros((TOK, HEAD_SIZE), F32)
    for h in range(KEY_VALUE_HEADS):
        x = k_vm[h].astype(F32)
        acc = acc + x * x
    mean_sq = jnp.sum(acc, axis=1, keepdims=True) * (1.0 / (KEY_VALUE_HEADS * HEAD_SIZE))
    rkb[...] = jnp.broadcast_to(lax.rsqrt(mean_sq + NORM_EPS), (TOK, HEAD_SIZE))
    for table in tables:
        table.wait()
    key_rotary(0)
    key_rotary(1)

    @pl.loop(0, KEY_VALUE_HEADS)
    def _(h):
        normed = k_vm[h].astype(F32) * rkb[...] * kg_ref[pl.ds(h, 1), :]
        kv[h, 0, 0:TOK] = (normed * cosk[0:TOK] + swap_halves(normed) * sink[0:TOK]).astype(BF16)
        to_across(0, h).start()
        to_partner(0, h).start()

        @pl.when(h < KEY_VALUE_HEADS - AHEAD)
        def _():
            values_out(h + AHEAD)

    cq[...] = cosk[0:TOK] * SCALE
    sq[...] = sink[0:TOK] * SCALE
    for index in range(2, SPANS):
        key_rotary(index)

    first = lane < SPAN
    query_span = jnp.where(first, spans[0], spans[1])
    doc_row = jnp.zeros((8, TOK), F32)
    for part in range(LENGTH // TOK):
        row = seg_ref[pl.ds(seq * (LENGTH // TOK) + part, 1), :].astype(F32)
        segcol[part * TOK : (part + 1) * TOK, :] = jnp.transpose(
            jnp.broadcast_to(row, (TOK, TOK))
        )
        row = jnp.broadcast_to(row, (8, TOK))
        turned = pltpu.roll(row, SPAN, 1)
        doc_row = jnp.where(query_span == 2 * part, jnp.where(first, row, turned), doc_row)
        doc_row = jnp.where(query_span == 2 * part + 1, jnp.where(first, turned, row), doc_row)
    doc_row = doc_row[0:1, :]
    pos_row = (query_span * SPAN + jnp.bitwise_and(lane, SPAN - 1))[0:1, :]
    for index, span in enumerate(spans):
        doc_col = pick(span, segcol)
        pos_col = span[0:1, :] * SPAN + sub_iota
        allowed = (doc_col == doc_row) & (pos_col <= pos_row)
        bias[index * SPAN : (index + 1) * SPAN, :] = jnp.where(allowed, 0.0, -jnp.inf)

    pltpu.make_async_copy(q_vm, q_vm, kin_sem.at[1]).wait()
    inner[...] = jnp.zeros((TOK, HEAD_SIZE), F32)

    @pl.loop(0, KEY_VALUE_HEADS)
    def _(h):
        total = inner[...]
        for j in range(HEADS_PER):
            x = q_vm[h, j * TOK : (j + 1) * TOK].astype(F32)
            total = total + x * x
        inner[...] = total

    mean_sq = jnp.sum(inner[...], axis=1, keepdims=True) * (1.0 / (QUERY_HEADS * HEAD_SIZE))
    rqb[...] = jnp.broadcast_to(lax.rsqrt(mean_sq + NORM_EPS), (TOK, HEAD_SIZE))
    inner[...] = jnp.zeros((TOK, HEAD_SIZE), F32)

    def take(h):
        to_across(0, h).wait_recv()
        to_across(1, h).wait_recv()
        forward(h).start()

    @pl.loop(0, KEY_VALUE_HEADS)
    def _(h):
        for j in range(HEADS_PER):
            rows = slice(j * TOK, (j + 1) * TOK)
            normed = q_vm[h, rows].astype(F32) * rqb[...] * qg_ref[pl.ds(h * HEADS_PER + j, 1), :]
            qr[h, rows] = (
                normed * cosk[0:TOK] + swap_halves(normed) * sink[0:TOK]
            ).astype(BF16)

    def add_and_send(h):
        grads_to_partner(h).wait_recv()
        for s in range(2):
            si[h, s] = (mid[h, s] + rd[h, s, TOK : 2 * TOK]).astype(BF16)
        grads_across(h).start()

    def shard_out(h):
        return pltpu.make_async_remote_copy(
            gpart.at[h], rs.at[rank], rs_send.at[h], rs_recv.at[rank],
            device_id=rank_peer(h), device_id_type=MESH,
        )

    def shard_got(source):
        return pltpu.make_async_remote_copy(
            gpart.at[0], rs.at[source], rs_send.at[0], rs_recv.at[source],
            device_id=rank_peer(source), device_id_type=MESH,
        )

    def plane_out(late, d):
        other = jnp.bitwise_xor(rank, d)
        return pltpu.make_async_remote_copy(
            gpart.at[EARLY + late], pf.at[late, rank], pf_send.at[late, d], pf_recv.at[late, rank],
            device_id=rank_peer(other), device_id_type=MESH,
        )

    def plane_got(late, d):
        other = jnp.bitwise_xor(rank, d)
        return pltpu.make_async_remote_copy(
            gpart.at[EARLY + late], pf.at[late, other], pf_send.at[late, d], pf_recv.at[late, other],
            device_id=rank_peer(other), device_id_type=MESH,
        )

    def z_copy(buffer, send, recv, d, source):
        return pltpu.make_async_remote_copy(
            buffer.at[source], buffer.at[source], send.at[d], recv.at[source],
            device_id={"context_1": lax.rem(zi + d, nz)}, device_id_type=MESH,
        )

    def z_out(d):
        return z_copy(za, za_send, za_recv, d, zi)

    def z_got(d):
        return z_copy(za, za_send, za_recv, d, lax.rem(zi + d, nz))

    def late_out(d):
        return z_copy(zf, zf_send, zf_recv, d, zi)

    def late_got(d):
        return z_copy(zf, zf_send, zf_recv, d, lax.rem(zi + d, nz))

    def total_out(d):
        other = jnp.bitwise_xor(rank, d)
        return pltpu.make_async_remote_copy(
            ag.at[rank], ag.at[rank], ag_send.at[d], ag_recv.at[rank],
            device_id=rank_peer(other), device_id_type=MESH,
        )

    def total_got(source):
        return pltpu.make_async_remote_copy(
            ag.at[source], ag.at[source], ag_send.at[0], ag_recv.at[source],
            device_id=rank_peer(source), device_id_type=MESH,
        )

    far_first = sorted(range(1, nz), key=lambda d: -min(d, nz - d))
    owner = rank < EARLY

    def shards_over_z():
        @pl.when(owner)
        def _():
            rs[rank] = gpart[rank]
            for d in range(1, nx * nc):
                shard_got(jnp.bitwise_xor(rank, d)).wait_recv()
            za[zi] = jnp.sum(rs[...], axis=0)
            for d in far_first:
                z_out(d).start()

    CH = 64
    nt = (((1,), (1,)), ((), ()))
    tn = (((0,), (0,)), ((), ()))
    nn = (((1,), (0,)), ((), ()))

    def arrived(h):
        to_partner(0, h).wait_recv()
        to_partner(1, h).wait_recv()
        forward(h).wait_recv()
        pltpu.make_async_copy(g_vm.at[h], g_vm.at[h], in_sem.at[h]).wait()

    slots = ((st0, dp0, tops0), (st1, dp1, tops1))

    PARTS = ((0, 2), (2, 4), (4, 5))

    def scores(h, slot, parts=PARTS):
        st, dp, tops = slots[slot]
        for lo, hi in parts:
            part = slice(lo * TOK, hi * TOK)
            raw = lax.dot_general(kv[h, 0], qr[h, part], nt, preferred_element_type=F32)
            st[:, part] = raw
            for j in range(lo, hi):
                cols = slice((j - lo) * TOK, (j - lo + 1) * TOK)
                top = jnp.full((8, TOK), -jnp.inf, F32)
                for c in range(LENGTH // CH):
                    rows = slice(c * CH, (c + 1) * CH)
                    masked = raw[rows, cols] + bias[rows, :]
                    top = jnp.maximum(top, jnp.max(masked.reshape(CH // 8, 8, TOK), axis=0))
                tops[j : j + 1, :] = jnp.max(top, axis=0, keepdims=True) * SCALE2
            dp[:, part] = lax.dot_general(kv[h, 1], g_vm[h, part], nt, preferred_element_type=F32)

    def softmax(j, slot):
        st, dp, tops = slots[slot]
        cols = slice(j * TOK, (j + 1) * TOK)
        top = tops[j : j + 1, :]
        weight = jnp.zeros((8, TOK), F32)
        delta = jnp.zeros((8, TOK), F32)
        for c in range(LENGTH // CH):
            rows = slice(c * CH, (c + 1) * CH)
            p = jnp.exp2((st[rows, cols] + bias[rows, :]) * SCALE2 - top)
            st[rows, cols] = p
            weight = weight + jnp.sum(p.reshape(CH // 8, 8, TOK), axis=0)
            delta = delta + jnp.sum((p * dp[rows, cols]).reshape(CH // 8, 8, TOK), axis=0)
        norm = 1.0 / jnp.sum(weight, axis=0, keepdims=True)
        delta = jnp.sum(delta, axis=0, keepdims=True) * norm
        for c in range(LENGTH // CH):
            rows = slice(c * CH, (c + 1) * CH)
            p = st[rows, cols] * norm
            pt[rows, cols] = p.astype(BF16)
            ds[rows, cols] = (p * (dp[rows, cols] - delta)).astype(BF16)

    def query_grads(h):
        dq = lax.dot_general(ds[...], kv[h, 0], tn, preferred_element_type=F32)
        along = jnp.zeros((TOK, HEAD_SIZE), F32)
        for j in range(HEADS_PER):
            d_part = dq[j * TOK : (j + 1) * TOK]
            d_part = d_part * cq[...] - swap_halves(d_part) * sq[...]
            dqw[h, j * TOK : (j + 1) * TOK] = d_part
            d_part = d_part * q_vm[h, j * TOK : (j + 1) * TOK].astype(F32)
            gpart[h, j : j + 1, :] = jnp.sum(d_part * rqb[...], axis=0, keepdims=True)
            along = along + d_part * qg_ref[pl.ds(h * HEADS_PER + j, 1), :]
        inner[...] = inner[...] + along

    def key_grads(h):
        dk = lax.dot_general(ds[...], qr[h], nn, preferred_element_type=F32)
        dv = lax.dot_general(pt[...], g_vm[h], nn, preferred_element_type=F32)
        own[h, 0] = dk[0:TOK]
        mid[h, 0] = dk[TOK : 2 * TOK]
        sd[h, 0] = dk[2 * TOK :]
        total = jnp.zeros((8, HEAD_SIZE), F32)
        for c in range(4):
            rows = slice(c * TOK, (c + 1) * TOK)
            d_part = dk[rows]
            k_part = kv[h, 0, rows].astype(F32)
            d_part = d_part * cosk[rows] - swap_halves(d_part) * sink[rows]
            k_part = k_part * cosk[rows] - swap_halves(k_part) * sink[rows]
            total = total + jnp.sum((d_part * k_part).reshape(TOK // 8, 8, HEAD_SIZE), axis=0)
        gpart[h, HEADS_PER : HEADS_PER + 1, :] = (
            jnp.sum(total, axis=0, keepdims=True) * SCALE / kg_ref[pl.ds(h, 1), :]
        )
        gpart[h, HEADS_PER + 1 :, :] = jnp.zeros((7 - HEADS_PER, HEAD_SIZE), F32)

        own[h, 1] = dv[0:TOK]
        mid[h, 1] = dv[TOK : 2 * TOK]
        sd[h, 1] = dv[2 * TOK :]

    def step(h, slot, first=None, last=False):
        if first is None:
            add_and_send(h - 2)
        else:
            @pl.when(jnp.logical_not(first))
            def _():
                add_and_send(h - 2)

        if not last:
            arrived(h + 1)
            if not isinstance(h, int):
                take(h + 2)
        for lo, hi in PARTS:
            if not last:
                scores(h + 1, 1 - slot, ((lo, hi),))
            for j in range(lo, hi):
                softmax(j, slot)
        query_grads(h)
        key_grads(h)
        if isinstance(h, int):
            for d in range(1, nx * nc):
                plane_out(h - EARLY, d).start()
        else:
            @pl.when(rank != h)
            def _():
                shard_out(h).start()

        grads_to_partner(h).start()

    for h in range(2):
        take(h)
    arrived(0)
    scores(0, 0)

    @pl.loop(0, EARLY // 2)
    def _(i):
        step(2 * i, 0, first=i == 0)
        step(2 * i + 1, 1, first=i == 0)

    last = KEY_VALUE_HEADS - 1
    step(last - 1, 0)
    step(last, 1, last=True)
    add_and_send(last - 1)
    shards_over_z()

    for late in range(LATE):
        pf[late, rank] = gpart[EARLY + late]
        for d in range(1, nx * nc):
            plane_got(late, d).wait_recv()
        zf[zi, late] = jnp.sum(pf[late], axis=0)
    for d in far_first:
        late_out(d).start()
    add_and_send(last)

    inner_q = jnp.sum(inner[...], axis=1, keepdims=True) * (1.0 / (QUERY_HEADS * HEAD_SIZE))
    cube = rqb[...] * rqb[...] * rqb[...] * inner_q
    inner[...] = cube

    def q_out(h, j):
        cols = pl.ds(pl.multiple_of((h * HEADS_PER + j) * HEAD_SIZE, HEAD_SIZE), HEAD_SIZE)
        rows = pl.ds(j * TOK, TOK)
        return pltpu.make_async_copy(outb.at[h, rows], qgrad_hbm.at[:, cols], out_sem.at[h, j])

    @pl.loop(0, KEY_VALUE_HEADS)
    def _(h):
        for j in range(HEADS_PER):
            rows = slice(j * TOK, (j + 1) * TOK)
            x = q_vm[h, rows].astype(F32)
            weighted = dqw[h, rows] * qg_ref[pl.ds(h * HEADS_PER + j, 1), :]
            outb[h, rows] = (rqb[...] * weighted - x * inner[...]).astype(BF16)
            q_out(h, j).start()

    @pl.when(owner)
    def _():
        for d in range(1, nz):
            z_got(d).wait_recv()
        ag[rank] = jnp.sum(za[...], axis=0)
        for d in range(1, nx * nc):
            total_out(d).start()

    def k_out(h, s, out):
        cols = pl.ds(pl.multiple_of(h * HEAD_SIZE, HEAD_SIZE), HEAD_SIZE)
        return pltpu.make_async_copy(si.at[h, s], out.at[:, cols], out_sem.at[h, HEADS_PER + s])

    inner[...] = jnp.zeros((TOK, HEAD_SIZE), F32)

    @pl.loop(0, KEY_VALUE_HEADS)
    def _(h):
        grads_across(h).wait()
        d_part = own[h, 0] + rd[h, 0, 0:TOK] + ri[h, 0].astype(F32)
        d_part = d_part * cq[...] - swap_halves(d_part) * sq[...]
        weighted = d_part * kg_ref[pl.ds(h, 1), :]
        dkw[h] = weighted
        inner[...] = inner[...] + weighted * k_vm[h].astype(F32)
        si[h, 1] = (own[h, 1] + rd[h, 1, 0:TOK] + ri[h, 1].astype(F32)).astype(BF16)
        k_out(h, 1, vgrad_hbm).start()

    inner_k = jnp.sum(inner[...], axis=1, keepdims=True) * (1.0 / (KEY_VALUE_HEADS * HEAD_SIZE))
    inner[...] = rkb[...] * rkb[...] * rkb[...] * inner_k

    @pl.loop(0, KEY_VALUE_HEADS)
    def _(h):
        si[h, 0] = (rkb[...] * dkw[h] - k_vm[h].astype(F32) * inner[...]).astype(BF16)
        k_out(h, 0, kgrad_hbm).start()

    for d in range(1, nz):
        late_got(d).wait_recv()
    late_totals = jnp.sum(zf[...], axis=0)
    for source in range(EARLY):
        @pl.when(rank != source)
        def _():
            total_got(source).wait_recv()
    for h in range(KEY_VALUE_HEADS):
        total = ag[h] if h < EARLY else late_totals[h - EARLY]
        qgain_ref[h * HEADS_PER : (h + 1) * HEADS_PER, :] = total[0:HEADS_PER, :]
        kgain_ref[h : h + 1, :] = total[HEADS_PER : HEADS_PER + 1, :]

    @pl.loop(0, KEY_VALUE_HEADS)
    def _(h):
        for s in range(2):
            to_across(s, h).wait_send()
            to_partner(s, h).wait_send()
        forward(h).wait_send()
        grads_to_partner(h).wait_send()
        for j in range(HEADS_PER):
            q_out(h, j).wait()
        k_out(h, 0, kgrad_hbm).wait()
        k_out(h, 1, vgrad_hbm).wait()

    for h in range(EARLY):
        @pl.when(rank != h)
        def _():
            shard_out(h).wait_send()
    for d in range(1, nx * nc):
        for late in range(LATE):
            plane_out(late, d).wait_send()
    for d in range(1, nz):
        late_out(d).wait_send()

    @pl.when(owner)
    def _():
        for d in range(1, nx * nc):
            total_out(d).wait_send()
        for d in range(1, nz):
            z_out(d).wait_send()


def settle(*refs):
    copies = [
        pltpu.make_async_copy(refs[i], refs[5 + i], refs[10].at[i]) for i in range(5)
    ]
    for copy in copies:
        copy.start()
    for copy in copies:
        copy.wait()


def body(nx, nz, nc, query_proj, key_proj, values, grad_out, query_gain, key_gain, segments, layout):
    cos_table, sin_table = rope_tables()
    assert nx * nc == KEY_VALUE_HEADS
    kvh, hs = KEY_VALUE_HEADS, HEAD_SIZE
    any_spec = pl.BlockSpec(memory_space=pl.ANY)
    vm_spec = pl.BlockSpec(memory_space=pltpu.VMEM)
    dma = pltpu.SemaphoreType.DMA
    out = pl.pallas_call(
        functools.partial(kernel, nx, nz, nc),
        out_shape=(
            jax.ShapeDtypeStruct(query_proj.shape, BF16),
            jax.ShapeDtypeStruct(key_proj.shape, BF16),
            jax.ShapeDtypeStruct(values.shape, BF16),
            jax.ShapeDtypeStruct((QUERY_HEADS, hs), F32),
            jax.ShapeDtypeStruct((kvh, hs), F32),
        ),
        in_specs=[pl.BlockSpec(memory_space=pltpu.HBM)] * 7 + [vm_spec] * 2 + [pl.BlockSpec(memory_space=pltpu.SMEM)],
        out_specs=(any_spec, any_spec, any_spec, vm_spec, vm_spec),
        scratch_shapes=[
            pltpu.VMEM((LENGTH, hs), F32),
            pltpu.VMEM((LENGTH, hs), F32),
            pltpu.VMEM((segments.shape[0] // TOK, TOK), jnp.int32),
            pltpu.VMEM((kvh, QROWS, hs), BF16),
            pltpu.VMEM((kvh, QROWS, hs), BF16),
            pltpu.VMEM((kvh, TOK, hs), BF16),
            pltpu.VMEM((kvh, 2, LENGTH, hs), BF16),
            pltpu.VMEM((kvh, QROWS, hs), BF16),
            pltpu.VMEM((LENGTH, QROWS), F32),
            pltpu.VMEM((LENGTH, QROWS), F32),
            pltpu.VMEM((LENGTH, QROWS), F32),
            pltpu.VMEM((LENGTH, QROWS), F32),
            pltpu.VMEM((LENGTH, QROWS), BF16),
            pltpu.VMEM((LENGTH, QROWS), BF16),
            pltpu.VMEM((kvh, QROWS, hs), F32),
            pltpu.VMEM((kvh, TOK, hs), F32),
            pltpu.VMEM((LENGTH, TOK), F32),
            pltpu.VMEM((LENGTH, TOK), F32),
            pltpu.VMEM((LENGTH, hs), F32),
            pltpu.VMEM((LENGTH, hs), F32),
            pltpu.VMEM((TOK, hs), F32),
            pltpu.VMEM((TOK, hs), F32),
            pltpu.VMEM((TOK, hs), F32),
            pltpu.VMEM((TOK, hs), F32),
            pltpu.VMEM((TOK, hs), F32),
            pltpu.VMEM((kvh, 2, TOK, hs), F32),
            pltpu.VMEM((kvh, 2, TOK, hs), F32),
            pltpu.VMEM((kvh, 2, 2 * TOK, hs), F32),
            pltpu.VMEM((kvh, 2, 2 * TOK, hs), F32),
            pltpu.VMEM((kvh, 2, TOK, hs), BF16),
            pltpu.VMEM((kvh, 2, TOK, hs), BF16),
            pltpu.VMEM((kvh, QROWS, hs), BF16),
            pltpu.VMEM((8, TOK), F32),
            pltpu.VMEM((8, TOK), F32),
            pltpu.VMEM((kvh, 8, hs), F32),
            pltpu.VMEM((kvh, 8, hs), F32),
            pltpu.VMEM((LATE, kvh, 8, hs), F32),
            pltpu.VMEM((nz, 8, hs), F32),
            pltpu.VMEM((nz, LATE, 8, hs), F32),
            pltpu.VMEM((kvh, 8, hs), F32),
            dma((kvh,)), dma((2,)), dma((kvh,)), dma((3,)),
            dma((2, kvh)), dma((2, kvh)), dma((2, kvh)), dma((2, kvh)), dma((kvh,)), dma((kvh,)),
            dma((kvh,)), dma((kvh,)), dma((kvh,)), dma((kvh,)),
            dma((kvh,)), dma((kvh,)), dma((LATE, kvh)), dma((LATE, kvh)),
            dma((nz,)), dma((nz,)), dma((nz,)), dma((nz,)), dma((kvh,)), dma((kvh,)),
            dma((kvh, HEADS_PER + 2)),
        ],
        compiler_params=pltpu.CompilerParams(
            collective_id=0, has_side_effects=True, vmem_limit_bytes=36 * 1024 * 1024
        ),
    )(
        *(
            pltpu.with_memory_space_constraint(x, pltpu.HBM)
            for x in (
                query_proj, key_proj, values, grad_out,
                jnp.asarray(cos_table), jnp.asarray(sin_table), segments.reshape(-1, TOK),
                query_gain.reshape(QUERY_HEADS, hs), key_gain.reshape(kvh, hs), layout,
            )
        ),
    )
    out = pl.pallas_call(
        settle,
        out_shape=[jax.ShapeDtypeStruct(o.shape, o.dtype) for o in out],
        in_specs=[any_spec] * 5,
        out_specs=[any_spec] * 5,
        scratch_shapes=[dma((5,))],
        compiler_params=pltpu.CompilerParams(vmem_limit_bytes=1024 * 1024),
    )(*out)
    return out[0], out[1], out[2], out[3].reshape(-1), out[4].reshape(-1)


def solution(mesh):
    nx, nz, nc = 4, 16, 2
    split = Mesh(mesh.devices.reshape(mesh.shape["groups"], nx, nz, nc), GROUPS_CONTEXT)
    tokens = P(GROUPS_CONTEXT, None)
    return jax.shard_map(
        functools.partial(body, nx, nz, nc),
        mesh=split,
        in_specs=(tokens, tokens, tokens, tokens, P(), P(), P("groups"), P("groups")),
        out_specs=(tokens, tokens, tokens, P("groups"), P("groups")),
        check_vma=False,
    )
```

```python
import functools
import math

import jax
import jax.numpy as jnp
import numpy as np
from jax import lax
from jax.experimental import pallas as pl
from jax.experimental.pallas import tpu as pltpu
from jax.sharding import Mesh
from jax.sharding import PartitionSpec as P

QUERY_HEADS = 40
KEY_VALUE_HEADS = 8
HEADS_PER = QUERY_HEADS // KEY_VALUE_HEADS
HEAD_SIZE = 128
SPAN = 64
LENGTH = 512
SPANS = LENGTH // SPAN
TOK = 128
QROWS = HEADS_PER * TOK
CONTEXT = ("context_0", "context_1", "context_2")
GROUPS_CONTEXT = ("groups", "context_0", "context_1", "context_2")
NORM_EPS = 1e-06
ROPE_BASE = 500000.0
SCALE = HEAD_SIZE ** (-0.5)
SCALE2 = SCALE * math.log2(math.e)
MESH = pl.DeviceIdType.MESH
F32 = jnp.float32
BF16 = jnp.bfloat16


def rope_tables():
    half = HEAD_SIZE // 2
    inv_freq = np.power(ROPE_BASE, -2.0 * np.arange(half) / HEAD_SIZE)
    angles = np.arange(LENGTH)[:, None] * inv_freq[None, :]
    cosine, sine = np.cos(angles), np.sin(angles)
    return (
        np.concatenate([cosine, cosine], axis=1).astype(np.float32),
        np.concatenate([-sine, sine], axis=1).astype(np.float32),
    )


def swap_halves(x):
    return pltpu.roll(x, HEAD_SIZE // 2, 1)


def kernel(
    nx, nz, nc,
    q_hbm, k_hbm, v_hbm, g_hbm, cos_hbm, sin_hbm, seg_hbm, qg_ref, kg_ref, lay_ref,
    qgrad_hbm, kgrad_hbm, vgrad_hbm, qgain_ref, kgain_ref,
    cos_ref, sin_ref, seg_ref,
    q_vm, g_vm, k_vm, kv, qr, st0, st1, dp0, dp1, pt, ds, dqw, dkw,
    bias, segcol, cosk, sink, cq, sq, rqb, rkb, inner,
    own, mid, sd, rd, si, ri, outb,
    tops0, tops1, gpart, rs, za, ag,
    in_sem, kin_sem, vin_sem, tab_sem,
    z_send, z_recv, c_send, c_recv, f_send, f_recv,
    d_send, d_recv, i_send, i_recv,
    rs_send, rs_recv, za_send, za_recv, ag_send, ag_recv,
    out_sem,
):
    xi = lax.axis_index("context_0")
    zi = lax.axis_index("context_1")
    ci = lax.axis_index("context_2")
    rank = xi * nc + ci
    seq = xi * (nz // 2) + zi // 2
    z_flip = zi + 1 - 2 * lax.rem(zi, 2)
    partner = {"context_2": 1 - ci}
    across = {"context_1": z_flip}

    def rank_peer(other):
        return {"context_0": other // nc, "context_2": lax.rem(other, nc)}

    def k_in(h):
        cols = pl.ds(pl.multiple_of(h * HEAD_SIZE, HEAD_SIZE), HEAD_SIZE)
        return pltpu.make_async_copy(k_hbm.at[:, cols], k_vm.at[h], kin_sem.at[0])

    def v_in(h):
        cols = pl.ds(pl.multiple_of(h * HEAD_SIZE, HEAD_SIZE), HEAD_SIZE)
        return pltpu.make_async_copy(v_hbm.at[:, cols], kv.at[h, 1, 0:TOK], vin_sem.at[h])

    def q_in(h, j):
        cols = pl.ds(pl.multiple_of((h * HEADS_PER + j) * HEAD_SIZE, HEAD_SIZE), HEAD_SIZE)
        rows = pl.ds(j * TOK, TOK)
        return pltpu.make_async_copy(q_hbm.at[:, cols], q_vm.at[h, rows], kin_sem.at[1])

    def g_in(h, j):
        cols = pl.ds(pl.multiple_of((h * HEADS_PER + j) * HEAD_SIZE, HEAD_SIZE), HEAD_SIZE)
        rows = pl.ds(j * TOK, TOK)
        return pltpu.make_async_copy(g_hbm.at[:, cols], g_vm.at[h, rows], in_sem.at[h])

    tables = [
        pltpu.make_async_copy(source, target, tab_sem.at[index])
        for index, (source, target) in enumerate(
            ((cos_hbm, cos_ref), (sin_hbm, sin_ref), (seg_hbm, seg_ref))
        )
    ]
    for h in range(KEY_VALUE_HEADS):
        v_in(h).start()
        k_in(h).start()
    for table in tables:
        table.start()

    barrier = pltpu.get_barrier_semaphore()
    for d in range(1, nx * nc):
        pl.semaphore_signal(
            barrier, inc=1, device_id=rank_peer(jnp.bitwise_xor(rank, d)), device_id_type=MESH
        )
    for d in range(1, nz):
        pl.semaphore_signal(
            barrier, inc=1, device_id={"context_1": lax.rem(zi + d, nz)}, device_id_type=MESH
        )

    my_local = 2 * lax.rem(zi, 2) + ci
    sub_iota = lax.broadcasted_iota(jnp.int32, (SPAN, TOK), 0)
    lane = lax.broadcasted_iota(jnp.int32, (8, TOK), 1)
    spans = []
    for flip in (0, 2, 1, 3):
        holder = jnp.bitwise_xor(my_local, flip)
        for part in range(2):
            slot = lay_ref[seq * SPANS + 2 * holder + part]
            spans.append(jnp.bitwise_and(jnp.full((8, TOK), slot, jnp.int32), SPANS - 1))

    def pick(span, table):
        chosen = table[0:SPAN, :]
        wide = jnp.concatenate([span] * (SPAN // 8), axis=0)
        for at in range(1, SPANS):
            chosen = jnp.where(wide == at, table[at * SPAN : (at + 1) * SPAN, :], chosen)
        return chosen

    def key_rotary(index):
        rows = slice(index * SPAN, (index + 1) * SPAN)
        cosk[rows, :] = pick(spans[index], cos_ref)
        sink[rows, :] = pick(spans[index], sin_ref)

    def to_across(s, h):
        return pltpu.make_async_remote_copy(
            kv.at[h, s, 0:TOK], kv.at[h, s, TOK : 2 * TOK], z_send.at[s, h], z_recv.at[s, h],
            device_id=across, device_id_type=MESH,
        )

    def to_partner(s, h):
        return pltpu.make_async_remote_copy(
            kv.at[h, s, 0:TOK], kv.at[h, s, 2 * TOK : 3 * TOK], c_send.at[s, h], c_recv.at[s, h],
            device_id=partner, device_id_type=MESH,
        )

    def forward(h):
        return pltpu.make_async_remote_copy(
            kv.at[h, :, TOK : 2 * TOK], kv.at[h, :, 3 * TOK : 4 * TOK], f_send.at[h], f_recv.at[h],
            device_id=partner, device_id_type=MESH,
        )

    def grads_to_partner(h):
        return pltpu.make_async_remote_copy(
            sd.at[h], rd.at[h], d_send.at[h], d_recv.at[h],
            device_id=partner, device_id_type=MESH,
        )

    def grads_across(h):
        return pltpu.make_async_remote_copy(
            si.at[h], ri.at[h], i_send.at[h], i_recv.at[h],
            device_id=across, device_id_type=MESH,
        )

    def values_out(h):
        v_in(h).wait()
        to_across(1, h).start()
        to_partner(1, h).start()

    AHEAD = 2
    pl.semaphore_wait(barrier, nx * nc - 1 + nz - 1)
    for h in range(AHEAD):
        values_out(h)

    @pl.loop(0, KEY_VALUE_HEADS)
    def _(h):
        for j in range(HEADS_PER):
            q_in(h, j).start()
            g_in(h, j).start()

    pltpu.make_async_copy(k_vm, k_vm, kin_sem.at[0]).wait()
    acc = jnp.zeros((TOK, HEAD_SIZE), F32)
    for h in range(KEY_VALUE_HEADS):
        x = k_vm[h].astype(F32)
        acc = acc + x * x
    mean_sq = jnp.sum(acc, axis=1, keepdims=True) * (1.0 / (KEY_VALUE_HEADS * HEAD_SIZE))
    rkb[...] = jnp.broadcast_to(lax.rsqrt(mean_sq + NORM_EPS), (TOK, HEAD_SIZE))
    for table in tables:
        table.wait()
    key_rotary(0)
    key_rotary(1)

    @pl.loop(0, KEY_VALUE_HEADS)
    def _(h):
        normed = k_vm[h].astype(F32) * rkb[...] * kg_ref[pl.ds(h, 1), :]
        kv[h, 0, 0:TOK] = (normed * cosk[0:TOK] + swap_halves(normed) * sink[0:TOK]).astype(BF16)
        to_across(0, h).start()
        to_partner(0, h).start()

        @pl.when(h < KEY_VALUE_HEADS - AHEAD)
        def _():
            values_out(h + AHEAD)

    cq[...] = cosk[0:TOK] * SCALE
    sq[...] = sink[0:TOK] * SCALE
    for index in range(2, SPANS):
        key_rotary(index)

    first = lane < SPAN
    query_span = jnp.where(first, spans[0], spans[1])
    doc_row = jnp.zeros((8, TOK), F32)
    for part in range(LENGTH // TOK):
        row = seg_ref[pl.ds(seq * (LENGTH // TOK) + part, 1), :].astype(F32)
        segcol[part * TOK : (part + 1) * TOK, :] = jnp.transpose(
            jnp.broadcast_to(row, (TOK, TOK))
        )
        row = jnp.broadcast_to(row, (8, TOK))
        turned = pltpu.roll(row, SPAN, 1)
        doc_row = jnp.where(query_span == 2 * part, jnp.where(first, row, turned), doc_row)
        doc_row = jnp.where(query_span == 2 * part + 1, jnp.where(first, turned, row), doc_row)
    doc_row = doc_row[0:1, :]
    pos_row = (query_span * SPAN + jnp.bitwise_and(lane, SPAN - 1))[0:1, :]
    for index, span in enumerate(spans):
        doc_col = pick(span, segcol)
        pos_col = span[0:1, :] * SPAN + sub_iota
        allowed = (doc_col == doc_row) & (pos_col <= pos_row)
        bias[index * SPAN : (index + 1) * SPAN, :] = jnp.where(allowed, 0.0, -jnp.inf)

    pltpu.make_async_copy(q_vm, q_vm, kin_sem.at[1]).wait()
    inner[...] = jnp.zeros((TOK, HEAD_SIZE), F32)

    @pl.loop(0, KEY_VALUE_HEADS)
    def _(h):
        total = inner[...]
        for j in range(HEADS_PER):
            x = q_vm[h, j * TOK : (j + 1) * TOK].astype(F32)
            total = total + x * x
        inner[...] = total

    mean_sq = jnp.sum(inner[...], axis=1, keepdims=True) * (1.0 / (QUERY_HEADS * HEAD_SIZE))
    rqb[...] = jnp.broadcast_to(lax.rsqrt(mean_sq + NORM_EPS), (TOK, HEAD_SIZE))
    inner[...] = jnp.zeros((TOK, HEAD_SIZE), F32)

    def take(h):
        to_across(0, h).wait_recv()
        to_across(1, h).wait_recv()
        forward(h).start()

    @pl.loop(0, KEY_VALUE_HEADS)
    def _(h):
        for j in range(HEADS_PER):
            rows = slice(j * TOK, (j + 1) * TOK)
            normed = q_vm[h, rows].astype(F32) * rqb[...] * qg_ref[pl.ds(h * HEADS_PER + j, 1), :]
            qr[h, rows] = (
                normed * cosk[0:TOK] + swap_halves(normed) * sink[0:TOK]
            ).astype(BF16)

    def add_and_send(h):
        grads_to_partner(h).wait_recv()
        for s in range(2):
            si[h, s] = (mid[h, s] + rd[h, s, TOK : 2 * TOK]).astype(BF16)
        grads_across(h).start()

    def shard_out(h):
        return pltpu.make_async_remote_copy(
            gpart.at[h], rs.at[rank], rs_send.at[h], rs_recv.at[rank],
            device_id=rank_peer(h), device_id_type=MESH,
        )

    def shard_got(source):
        return pltpu.make_async_remote_copy(
            gpart.at[0], rs.at[source], rs_send.at[0], rs_recv.at[source],
            device_id=rank_peer(source), device_id_type=MESH,
        )

    def z_copy(buffer, send, recv, d, source):
        return pltpu.make_async_remote_copy(
            buffer.at[source], buffer.at[source], send.at[d], recv.at[source],
            device_id={"context_1": lax.rem(zi + d, nz)}, device_id_type=MESH,
        )

    def z_out(d):
        return z_copy(za, za_send, za_recv, d, zi)

    def z_got(d):
        return z_copy(za, za_send, za_recv, d, lax.rem(zi + d, nz))

    def total_out(d):
        other = jnp.bitwise_xor(rank, d)
        return pltpu.make_async_remote_copy(
            ag.at[rank], ag.at[rank], ag_send.at[d], ag_recv.at[rank],
            device_id=rank_peer(other), device_id_type=MESH,
        )

    def total_got(source):
        return pltpu.make_async_remote_copy(
            ag.at[source], ag.at[source], ag_send.at[0], ag_recv.at[source],
            device_id=rank_peer(source), device_id_type=MESH,
        )

    near_first = sorted(range(1, nz), key=lambda d: min(d, nz - d))

    def shards_over_z():
        rs[rank] = gpart[rank]
        for d in range(1, nx * nc):
            shard_got(jnp.bitwise_xor(rank, d)).wait_recv()
        za[zi] = jnp.sum(rs[...], axis=0)
        for d in near_first:
            z_out(d).start()

    CH = 64
    nt = (((1,), (1,)), ((), ()))
    tn = (((0,), (0,)), ((), ()))
    nn = (((1,), (0,)), ((), ()))

    def arrived(h):
        to_partner(0, h).wait_recv()
        to_partner(1, h).wait_recv()
        forward(h).wait_recv()
        pltpu.make_async_copy(g_vm.at[h], g_vm.at[h], in_sem.at[h]).wait()

    slots = ((st0, dp0, tops0), (st1, dp1, tops1))

    PARTS = ((0, 2), (2, 4), (4, 5))

    def scores(h, slot, parts=PARTS):
        st, dp, tops = slots[slot]
        for lo, hi in parts:
            part = slice(lo * TOK, hi * TOK)
            raw = lax.dot_general(kv[h, 0], qr[h, part], nt, preferred_element_type=F32)
            st[:, part] = raw
            for j in range(lo, hi):
                cols = slice((j - lo) * TOK, (j - lo + 1) * TOK)
                top = jnp.full((8, TOK), -jnp.inf, F32)
                for c in range(LENGTH // CH):
                    rows = slice(c * CH, (c + 1) * CH)
                    masked = raw[rows, cols] + bias[rows, :]
                    top = jnp.maximum(top, jnp.max(masked.reshape(CH // 8, 8, TOK), axis=0))
                tops[j : j + 1, :] = jnp.max(top, axis=0, keepdims=True) * SCALE2
            dp[:, part] = lax.dot_general(kv[h, 1], g_vm[h, part], nt, preferred_element_type=F32)

    def softmax(j, slot):
        st, dp, tops = slots[slot]
        cols = slice(j * TOK, (j + 1) * TOK)
        top = tops[j : j + 1, :]
        weight = jnp.zeros((8, TOK), F32)
        delta = jnp.zeros((8, TOK), F32)
        for c in range(LENGTH // CH):
            rows = slice(c * CH, (c + 1) * CH)
            p = jnp.exp2((st[rows, cols] + bias[rows, :]) * SCALE2 - top)
            st[rows, cols] = p
            weight = weight + jnp.sum(p.reshape(CH // 8, 8, TOK), axis=0)
            delta = delta + jnp.sum((p * dp[rows, cols]).reshape(CH // 8, 8, TOK), axis=0)
        norm = 1.0 / jnp.sum(weight, axis=0, keepdims=True)
        delta = jnp.sum(delta, axis=0, keepdims=True) * norm
        for c in range(LENGTH // CH):
            rows = slice(c * CH, (c + 1) * CH)
            p = st[rows, cols] * norm
            pt[rows, cols] = p.astype(BF16)
            ds[rows, cols] = (p * (dp[rows, cols] - delta)).astype(BF16)

    def query_grads(h):
        dq = lax.dot_general(ds[...], kv[h, 0], tn, preferred_element_type=F32)
        along = jnp.zeros((TOK, HEAD_SIZE), F32)
        for j in range(HEADS_PER):
            d_part = dq[j * TOK : (j + 1) * TOK]
            d_part = d_part * cq[...] - swap_halves(d_part) * sq[...]
            dqw[h, j * TOK : (j + 1) * TOK] = d_part
            d_part = d_part * q_vm[h, j * TOK : (j + 1) * TOK].astype(F32)
            gpart[h, j : j + 1, :] = jnp.sum(d_part * rqb[...], axis=0, keepdims=True)
            along = along + d_part * qg_ref[pl.ds(h * HEADS_PER + j, 1), :]
        inner[...] = inner[...] + along

    def key_grads(h):
        dk = lax.dot_general(ds[...], qr[h], nn, preferred_element_type=F32)
        dv = lax.dot_general(pt[...], g_vm[h], nn, preferred_element_type=F32)
        own[h, 0] = dk[0:TOK]
        mid[h, 0] = dk[TOK : 2 * TOK]
        sd[h, 0] = dk[2 * TOK :]
        total = jnp.zeros((8, HEAD_SIZE), F32)
        for c in range(4):
            rows = slice(c * TOK, (c + 1) * TOK)
            d_part = dk[rows]
            k_part = kv[h, 0, rows].astype(F32)
            d_part = d_part * cosk[rows] - swap_halves(d_part) * sink[rows]
            k_part = k_part * cosk[rows] - swap_halves(k_part) * sink[rows]
            total = total + jnp.sum((d_part * k_part).reshape(TOK // 8, 8, HEAD_SIZE), axis=0)
        gpart[h, HEADS_PER : HEADS_PER + 1, :] = (
            jnp.sum(total, axis=0, keepdims=True) * SCALE / kg_ref[pl.ds(h, 1), :]
        )
        gpart[h, HEADS_PER + 1 :, :] = jnp.zeros((7 - HEADS_PER, HEAD_SIZE), F32)

        own[h, 1] = dv[0:TOK]
        mid[h, 1] = dv[TOK : 2 * TOK]
        sd[h, 1] = dv[2 * TOK :]

    def step(h, slot, first=None, last=False):
        if first is None:
            add_and_send(h - 2)
        else:
            @pl.when(jnp.logical_not(first))
            def _():
                add_and_send(h - 2)

        if not last:
            arrived(h + 1)
            if not isinstance(h, int):
                take(h + 2)
        for lo, hi in PARTS:
            if not last:
                scores(h + 1, 1 - slot, ((lo, hi),))
            for j in range(lo, hi):
                softmax(j, slot)
        query_grads(h)
        key_grads(h)
        @pl.when(rank != h)
        def _():
            shard_out(h).start()

        grads_to_partner(h).start()

    for h in range(2):
        take(h)
    arrived(0)
    scores(0, 0)

    last = KEY_VALUE_HEADS - 1

    @pl.loop(0, last // 2)
    def _(i):
        step(2 * i, 0, first=i == 0)
        step(2 * i + 1, 1, first=i == 0)

    step(last - 1, 0)
    step(last, 1, last=True)
    add_and_send(last - 1)
    shards_over_z()

    add_and_send(last)

    inner_q = jnp.sum(inner[...], axis=1, keepdims=True) * (1.0 / (QUERY_HEADS * HEAD_SIZE))
    cube = rqb[...] * rqb[...] * rqb[...] * inner_q
    inner[...] = cube

    def q_out(h, j):
        cols = pl.ds(pl.multiple_of((h * HEADS_PER + j) * HEAD_SIZE, HEAD_SIZE), HEAD_SIZE)
        rows = pl.ds(j * TOK, TOK)
        return pltpu.make_async_copy(outb.at[h, rows], qgrad_hbm.at[:, cols], out_sem.at[h, j])

    @pl.loop(0, KEY_VALUE_HEADS)
    def _(h):
        for j in range(HEADS_PER):
            rows = slice(j * TOK, (j + 1) * TOK)
            x = q_vm[h, rows].astype(F32)
            weighted = dqw[h, rows] * qg_ref[pl.ds(h * HEADS_PER + j, 1), :]
            outb[h, rows] = (rqb[...] * weighted - x * inner[...]).astype(BF16)
            q_out(h, j).start()

    for d in range(1, nz):
        z_got(d).wait_recv()
    ag[rank] = jnp.sum(za[...], axis=0)
    for d in range(1, nx * nc):
        total_out(d).start()

    def k_out(h, s, out):
        cols = pl.ds(pl.multiple_of(h * HEAD_SIZE, HEAD_SIZE), HEAD_SIZE)
        return pltpu.make_async_copy(si.at[h, s], out.at[:, cols], out_sem.at[h, HEADS_PER + s])

    inner[...] = jnp.zeros((TOK, HEAD_SIZE), F32)

    @pl.loop(0, KEY_VALUE_HEADS)
    def _(h):
        grads_across(h).wait()
        d_part = own[h, 0] + rd[h, 0, 0:TOK] + ri[h, 0].astype(F32)
        d_part = d_part * cq[...] - swap_halves(d_part) * sq[...]
        weighted = d_part * kg_ref[pl.ds(h, 1), :]
        dkw[h] = weighted
        inner[...] = inner[...] + weighted * k_vm[h].astype(F32)
        si[h, 1] = (own[h, 1] + rd[h, 1, 0:TOK] + ri[h, 1].astype(F32)).astype(BF16)
        k_out(h, 1, vgrad_hbm).start()

    inner_k = jnp.sum(inner[...], axis=1, keepdims=True) * (1.0 / (KEY_VALUE_HEADS * HEAD_SIZE))
    inner[...] = rkb[...] * rkb[...] * rkb[...] * inner_k

    @pl.loop(0, KEY_VALUE_HEADS)
    def _(h):
        si[h, 0] = (rkb[...] * dkw[h] - k_vm[h].astype(F32) * inner[...]).astype(BF16)
        k_out(h, 0, kgrad_hbm).start()

    for source in range(KEY_VALUE_HEADS):
        @pl.when(rank != source)
        def _():
            total_got(source).wait_recv()

        qgain_ref[source * HEADS_PER : (source + 1) * HEADS_PER, :] = ag[source, 0:HEADS_PER, :]
        kgain_ref[source : source + 1, :] = ag[source, HEADS_PER : HEADS_PER + 1, :]

    @pl.loop(0, KEY_VALUE_HEADS)
    def _(h):
        for s in range(2):
            to_across(s, h).wait_send()
            to_partner(s, h).wait_send()
        forward(h).wait_send()
        grads_to_partner(h).wait_send()
        for j in range(HEADS_PER):
            q_out(h, j).wait()
        k_out(h, 0, kgrad_hbm).wait()
        k_out(h, 1, vgrad_hbm).wait()

    for h in range(KEY_VALUE_HEADS):
        @pl.when(rank != h)
        def _():
            shard_out(h).wait_send()
    for d in range(1, nx * nc):
        total_out(d).wait_send()
    for d in range(1, nz):
        z_out(d).wait_send()


def settle(*refs):
    copies = [
        pltpu.make_async_copy(refs[i], refs[5 + i], refs[10].at[i]) for i in range(5)
    ]
    for copy in copies:
        copy.start()
    for copy in copies:
        copy.wait()


def body(nx, nz, nc, query_proj, key_proj, values, grad_out, query_gain, key_gain, segments, layout):
    cos_table, sin_table = rope_tables()
    assert nx * nc == KEY_VALUE_HEADS
    kvh, hs = KEY_VALUE_HEADS, HEAD_SIZE
    any_spec = pl.BlockSpec(memory_space=pl.ANY)
    vm_spec = pl.BlockSpec(memory_space=pltpu.VMEM)
    dma = pltpu.SemaphoreType.DMA
    out = pl.pallas_call(
        functools.partial(kernel, nx, nz, nc),
        out_shape=(
            jax.ShapeDtypeStruct(query_proj.shape, BF16),
            jax.ShapeDtypeStruct(key_proj.shape, BF16),
            jax.ShapeDtypeStruct(values.shape, BF16),
            jax.ShapeDtypeStruct((QUERY_HEADS, hs), F32),
            jax.ShapeDtypeStruct((kvh, hs), F32),
        ),
        in_specs=[pl.BlockSpec(memory_space=pltpu.HBM)] * 7 + [vm_spec] * 2 + [pl.BlockSpec(memory_space=pltpu.SMEM)],
        out_specs=(any_spec, any_spec, any_spec, vm_spec, vm_spec),
        scratch_shapes=[
            pltpu.VMEM((LENGTH, hs), F32),
            pltpu.VMEM((LENGTH, hs), F32),
            pltpu.VMEM((segments.shape[0] // TOK, TOK), jnp.int32),
            pltpu.VMEM((kvh, QROWS, hs), BF16),
            pltpu.VMEM((kvh, QROWS, hs), BF16),
            pltpu.VMEM((kvh, TOK, hs), BF16),
            pltpu.VMEM((kvh, 2, LENGTH, hs), BF16),
            pltpu.VMEM((kvh, QROWS, hs), BF16),
            pltpu.VMEM((LENGTH, QROWS), F32),
            pltpu.VMEM((LENGTH, QROWS), F32),
            pltpu.VMEM((LENGTH, QROWS), F32),
            pltpu.VMEM((LENGTH, QROWS), F32),
            pltpu.VMEM((LENGTH, QROWS), BF16),
            pltpu.VMEM((LENGTH, QROWS), BF16),
            pltpu.VMEM((kvh, QROWS, hs), F32),
            pltpu.VMEM((kvh, TOK, hs), F32),
            pltpu.VMEM((LENGTH, TOK), F32),
            pltpu.VMEM((LENGTH, TOK), F32),
            pltpu.VMEM((LENGTH, hs), F32),
            pltpu.VMEM((LENGTH, hs), F32),
            pltpu.VMEM((TOK, hs), F32),
            pltpu.VMEM((TOK, hs), F32),
            pltpu.VMEM((TOK, hs), F32),
            pltpu.VMEM((TOK, hs), F32),
            pltpu.VMEM((TOK, hs), F32),
            pltpu.VMEM((kvh, 2, TOK, hs), F32),
            pltpu.VMEM((kvh, 2, TOK, hs), F32),
            pltpu.VMEM((kvh, 2, 2 * TOK, hs), F32),
            pltpu.VMEM((kvh, 2, 2 * TOK, hs), F32),
            pltpu.VMEM((kvh, 2, TOK, hs), BF16),
            pltpu.VMEM((kvh, 2, TOK, hs), BF16),
            pltpu.VMEM((kvh, QROWS, hs), BF16),
            pltpu.VMEM((8, TOK), F32),
            pltpu.VMEM((8, TOK), F32),
            pltpu.VMEM((kvh, 8, hs), F32),
            pltpu.VMEM((kvh, 8, hs), F32),
            pltpu.VMEM((nz, 8, hs), F32),
            pltpu.VMEM((kvh, 8, hs), F32),
            dma((kvh,)), dma((2,)), dma((kvh,)), dma((3,)),
            dma((2, kvh)), dma((2, kvh)), dma((2, kvh)), dma((2, kvh)), dma((kvh,)), dma((kvh,)),
            dma((kvh,)), dma((kvh,)), dma((kvh,)), dma((kvh,)),
            dma((kvh,)), dma((kvh,)), dma((nz,)), dma((nz,)), dma((kvh,)), dma((kvh,)),
            dma((kvh, HEADS_PER + 2)),
        ],
        compiler_params=pltpu.CompilerParams(
            collective_id=0, has_side_effects=True, vmem_limit_bytes=36 * 1024 * 1024
        ),
    )(
        *(
            pltpu.with_memory_space_constraint(x, pltpu.HBM)
            for x in (
                query_proj, key_proj, values, grad_out,
                jnp.asarray(cos_table), jnp.asarray(sin_table), segments.reshape(-1, TOK),
                query_gain.reshape(QUERY_HEADS, hs), key_gain.reshape(kvh, hs), layout,
            )
        ),
    )
    out = pl.pallas_call(
        settle,
        out_shape=[jax.ShapeDtypeStruct(o.shape, o.dtype) for o in out],
        in_specs=[any_spec] * 5,
        out_specs=[any_spec] * 5,
        scratch_shapes=[dma((5,))],
        compiler_params=pltpu.CompilerParams(vmem_limit_bytes=1024 * 1024),
    )(*out)
    return out[0], out[1], out[2], out[3].reshape(-1), out[4].reshape(-1)


def solution(mesh):
    nx, nz, nc = 4, 16, 2
    split = Mesh(mesh.devices.reshape(mesh.shape["groups"], nx, nz, nc), GROUPS_CONTEXT)
    tokens = P(GROUPS_CONTEXT, None)
    return jax.shard_map(
        functools.partial(body, nx, nz, nc),
        mesh=split,
        in_specs=(tokens, tokens, tokens, tokens, P(), P(), P("groups"), P("groups")),
        out_specs=(tokens, tokens, tokens, P("groups"), P("groups")),
        check_vma=False,
    )
```

```python
import functools
import math

import jax
import jax.numpy as jnp
import numpy as np
from jax import lax
from jax.experimental import pallas as pl
from jax.experimental.pallas import tpu as pltpu
from jax.sharding import Mesh
from jax.sharding import PartitionSpec as P

QUERY_HEADS = 40
KEY_VALUE_HEADS = 8
HEADS_PER = QUERY_HEADS // KEY_VALUE_HEADS
HEAD_SIZE = 128
SPAN = 64
LENGTH = 512
SPANS = LENGTH // SPAN
TOK = 128
QROWS = HEADS_PER * TOK
CONTEXT = ("context_0", "context_1", "context_2")
GROUPS_CONTEXT = ("groups", "context_0", "context_1", "context_2")
NORM_EPS = 1e-06
ROPE_BASE = 500000.0
SCALE = HEAD_SIZE ** (-0.5)
SCALE2 = SCALE * math.log2(math.e)
MESH = pl.DeviceIdType.MESH
F32 = jnp.float32
BF16 = jnp.bfloat16


def rope_tables():
    half = HEAD_SIZE // 2
    inv_freq = np.power(ROPE_BASE, -2.0 * np.arange(half) / HEAD_SIZE)
    angles = np.arange(LENGTH)[:, None] * inv_freq[None, :]
    cosine, sine = np.cos(angles), np.sin(angles)
    return (
        np.concatenate([cosine, cosine], axis=1).astype(np.float32),
        np.concatenate([-sine, sine], axis=1).astype(np.float32),
    )


def swap_halves(x):
    return pltpu.roll(x, HEAD_SIZE // 2, 1)


def kernel(
    nx, nz, nc,
    q_hbm, k_hbm, v_hbm, g_hbm, cos_hbm, sin_hbm, seg_hbm, qg_ref, kg_ref, lay_ref,
    qgrad_hbm, kgrad_hbm, vgrad_hbm, qgain_ref, kgain_ref,
    cos_ref, sin_ref, seg_ref,
    q_vm, g_vm, k_vm, kv, qr, st0, st1, dp0, dp1, pt, ds, dqw, dkw,
    bias, segcol, cosk, sink, cq, sq, rqb, rkb, inner,
    own, mid, sd, rd, si, ri, outb,
    tops0, tops1, gpart, rs, za, ag,
    in_sem, kin_sem, vin_sem, tab_sem,
    z_send, z_recv, c_send, c_recv, f_send, f_recv,
    d_send, d_recv, i_send, i_recv,
    rs_send, rs_recv, za_send, za_recv, ag_send, ag_recv, near_sem,
    out_sem,
):
    xi = lax.axis_index("context_0")
    zi = lax.axis_index("context_1")
    ci = lax.axis_index("context_2")
    rank = xi * nc + ci
    seq = xi * (nz // 2) + zi // 2
    z_flip = zi + 1 - 2 * lax.rem(zi, 2)
    partner = {"context_2": 1 - ci}
    across = {"context_1": z_flip}

    def rank_peer(other):
        return {"context_0": other // nc, "context_2": lax.rem(other, nc)}

    def k_in(h):
        cols = pl.ds(pl.multiple_of(h * HEAD_SIZE, HEAD_SIZE), HEAD_SIZE)
        return pltpu.make_async_copy(k_hbm.at[:, cols], k_vm.at[h], kin_sem.at[0])

    def v_in(h):
        cols = pl.ds(pl.multiple_of(h * HEAD_SIZE, HEAD_SIZE), HEAD_SIZE)
        return pltpu.make_async_copy(v_hbm.at[:, cols], kv.at[h, 1, 0:TOK], vin_sem.at[h])

    def q_in(h, j):
        cols = pl.ds(pl.multiple_of((h * HEADS_PER + j) * HEAD_SIZE, HEAD_SIZE), HEAD_SIZE)
        rows = pl.ds(j * TOK, TOK)
        return pltpu.make_async_copy(q_hbm.at[:, cols], q_vm.at[h, rows], kin_sem.at[1])

    def g_in(h, j):
        cols = pl.ds(pl.multiple_of((h * HEADS_PER + j) * HEAD_SIZE, HEAD_SIZE), HEAD_SIZE)
        rows = pl.ds(j * TOK, TOK)
        return pltpu.make_async_copy(g_hbm.at[:, cols], g_vm.at[h, rows], in_sem.at[h])

    tables = [
        pltpu.make_async_copy(source, target, tab_sem.at[index])
        for index, (source, target) in enumerate(
            ((cos_hbm, cos_ref), (sin_hbm, sin_ref), (seg_hbm, seg_ref))
        )
    ]
    for h in range(KEY_VALUE_HEADS):
        v_in(h).start()
        k_in(h).start()
    for table in tables:
        table.start()

    barrier = pltpu.get_barrier_semaphore()
    for d in range(1, nx * nc):
        pl.semaphore_signal(
            barrier, inc=1, device_id=rank_peer(jnp.bitwise_xor(rank, d)), device_id_type=MESH
        )
    sides = sorted({1, nz - 1})
    for d in sides:
        pl.semaphore_signal(
            barrier, inc=1, device_id={"context_1": lax.rem(zi + d, nz)}, device_id_type=MESH
        )

    rounds = [1 << r for r in range(8) if 1 << r < nz // 2]

    def tell(r):
        for side, d in enumerate((rounds[r], nz - rounds[r])):
            pl.semaphore_signal(
                near_sem.at[r, side], inc=1,
                device_id={"context_1": lax.rem(zi + d, nz)}, device_id_type=MESH,
            )

    def heard(r):
        for side in range(2):
            pl.semaphore_wait(near_sem.at[r, side], 1)


    my_local = 2 * lax.rem(zi, 2) + ci
    sub_iota = lax.broadcasted_iota(jnp.int32, (SPAN, TOK), 0)
    lane = lax.broadcasted_iota(jnp.int32, (8, TOK), 1)
    spans = []
    for flip in (0, 2, 1, 3):
        holder = jnp.bitwise_xor(my_local, flip)
        for part in range(2):
            slot = lay_ref[seq * SPANS + 2 * holder + part]
            spans.append(jnp.bitwise_and(jnp.full((8, TOK), slot, jnp.int32), SPANS - 1))

    def pick(span, table):
        chosen = table[0:SPAN, :]
        wide = jnp.concatenate([span] * (SPAN // 8), axis=0)
        for at in range(1, SPANS):
            chosen = jnp.where(wide == at, table[at * SPAN : (at + 1) * SPAN, :], chosen)
        return chosen

    def key_rotary(index):
        rows = slice(index * SPAN, (index + 1) * SPAN)
        cosk[rows, :] = pick(spans[index], cos_ref)
        sink[rows, :] = pick(spans[index], sin_ref)

    def to_across(s, h):
        return pltpu.make_async_remote_copy(
            kv.at[h, s, 0:TOK], kv.at[h, s, TOK : 2 * TOK], z_send.at[s, h], z_recv.at[s, h],
            device_id=across, device_id_type=MESH,
        )

    def to_partner(s, h):
        return pltpu.make_async_remote_copy(
            kv.at[h, s, 0:TOK], kv.at[h, s, 2 * TOK : 3 * TOK], c_send.at[s, h], c_recv.at[s, h],
            device_id=partner, device_id_type=MESH,
        )

    def forward(h):
        return pltpu.make_async_remote_copy(
            kv.at[h, :, TOK : 2 * TOK], kv.at[h, :, 3 * TOK : 4 * TOK], f_send.at[h], f_recv.at[h],
            device_id=partner, device_id_type=MESH,
        )

    def grads_to_partner(h):
        return pltpu.make_async_remote_copy(
            sd.at[h], rd.at[h], d_send.at[h], d_recv.at[h],
            device_id=partner, device_id_type=MESH,
        )

    def grads_across(h):
        return pltpu.make_async_remote_copy(
            si.at[h], ri.at[h], i_send.at[h], i_recv.at[h],
            device_id=across, device_id_type=MESH,
        )

    def values_out(h):
        v_in(h).wait()
        to_across(1, h).start()
        to_partner(1, h).start()

    AHEAD = 2
    pl.semaphore_wait(barrier, nx * nc - 1 + len(sides))
    if rounds:
        tell(0)
    for h in range(AHEAD):
        values_out(h)

    @pl.loop(0, KEY_VALUE_HEADS)
    def _(h):
        for j in range(HEADS_PER):
            q_in(h, j).start()
            g_in(h, j).start()

    pltpu.make_async_copy(k_vm, k_vm, kin_sem.at[0]).wait()
    acc = jnp.zeros((TOK, HEAD_SIZE), F32)
    for h in range(KEY_VALUE_HEADS):
        x = k_vm[h].astype(F32)
        acc = acc + x * x
    mean_sq = jnp.sum(acc, axis=1, keepdims=True) * (1.0 / (KEY_VALUE_HEADS * HEAD_SIZE))
    rkb[...] = jnp.broadcast_to(lax.rsqrt(mean_sq + NORM_EPS), (TOK, HEAD_SIZE))
    for table in tables:
        table.wait()
    key_rotary(0)
    key_rotary(1)

    @pl.loop(0, KEY_VALUE_HEADS)
    def _(h):
        normed = k_vm[h].astype(F32) * rkb[...] * kg_ref[pl.ds(h, 1), :]
        kv[h, 0, 0:TOK] = (normed * cosk[0:TOK] + swap_halves(normed) * sink[0:TOK]).astype(BF16)
        to_across(0, h).start()
        to_partner(0, h).start()

        @pl.when(h < KEY_VALUE_HEADS - AHEAD)
        def _():
            values_out(h + AHEAD)

    cq[...] = cosk[0:TOK] * SCALE
    sq[...] = sink[0:TOK] * SCALE
    for index in range(2, SPANS):
        key_rotary(index)

    first = lane < SPAN
    query_span = jnp.where(first, spans[0], spans[1])
    doc_row = jnp.zeros((8, TOK), F32)
    for part in range(LENGTH // TOK):
        row = seg_ref[pl.ds(seq * (LENGTH // TOK) + part, 1), :].astype(F32)
        segcol[part * TOK : (part + 1) * TOK, :] = jnp.transpose(
            jnp.broadcast_to(row, (TOK, TOK))
        )
        row = jnp.broadcast_to(row, (8, TOK))
        turned = pltpu.roll(row, SPAN, 1)
        doc_row = jnp.where(query_span == 2 * part, jnp.where(first, row, turned), doc_row)
        doc_row = jnp.where(query_span == 2 * part + 1, jnp.where(first, turned, row), doc_row)
    doc_row = doc_row[0:1, :]
    pos_row = (query_span * SPAN + jnp.bitwise_and(lane, SPAN - 1))[0:1, :]
    for index, span in enumerate(spans):
        doc_col = pick(span, segcol)
        pos_col = span[0:1, :] * SPAN + sub_iota
        allowed = (doc_col == doc_row) & (pos_col <= pos_row)
        bias[index * SPAN : (index + 1) * SPAN, :] = jnp.where(allowed, 0.0, -jnp.inf)

    pltpu.make_async_copy(q_vm, q_vm, kin_sem.at[1]).wait()
    inner[...] = jnp.zeros((TOK, HEAD_SIZE), F32)

    @pl.loop(0, KEY_VALUE_HEADS)
    def _(h):
        total = inner[...]
        for j in range(HEADS_PER):
            x = q_vm[h, j * TOK : (j + 1) * TOK].astype(F32)
            total = total + x * x
        inner[...] = total

    mean_sq = jnp.sum(inner[...], axis=1, keepdims=True) * (1.0 / (QUERY_HEADS * HEAD_SIZE))
    rqb[...] = jnp.broadcast_to(lax.rsqrt(mean_sq + NORM_EPS), (TOK, HEAD_SIZE))
    inner[...] = jnp.zeros((TOK, HEAD_SIZE), F32)

    def take(h):
        to_across(0, h).wait_recv()
        to_across(1, h).wait_recv()
        forward(h).start()

    @pl.loop(0, KEY_VALUE_HEADS)
    def _(h):
        for j in range(HEADS_PER):
            rows = slice(j * TOK, (j + 1) * TOK)
            normed = q_vm[h, rows].astype(F32) * rqb[...] * qg_ref[pl.ds(h * HEADS_PER + j, 1), :]
            qr[h, rows] = (
                normed * cosk[0:TOK] + swap_halves(normed) * sink[0:TOK]
            ).astype(BF16)

    def add_and_send(h):
        grads_to_partner(h).wait_recv()
        for s in range(2):
            si[h, s] = (mid[h, s] + rd[h, s, TOK : 2 * TOK]).astype(BF16)
        grads_across(h).start()

    def shard_out(h):
        return pltpu.make_async_remote_copy(
            gpart.at[h], rs.at[rank], rs_send.at[h], rs_recv.at[rank],
            device_id=rank_peer(h), device_id_type=MESH,
        )

    def shard_got(source):
        return pltpu.make_async_remote_copy(
            gpart.at[0], rs.at[source], rs_send.at[0], rs_recv.at[source],
            device_id=rank_peer(source), device_id_type=MESH,
        )

    def z_copy(buffer, send, recv, d, source):
        return pltpu.make_async_remote_copy(
            buffer.at[source], buffer.at[source], send.at[d], recv.at[source],
            device_id={"context_1": lax.rem(zi + d, nz)}, device_id_type=MESH,
        )

    def z_out(d):
        return z_copy(za, za_send, za_recv, d, zi)

    def z_got(d):
        return z_copy(za, za_send, za_recv, d, lax.rem(zi + d, nz))

    def total_out(d):
        other = jnp.bitwise_xor(rank, d)
        return pltpu.make_async_remote_copy(
            ag.at[rank], ag.at[rank], ag_send.at[d], ag_recv.at[rank],
            device_id=rank_peer(other), device_id_type=MESH,
        )

    def total_got(source):
        return pltpu.make_async_remote_copy(
            ag.at[source], ag.at[source], ag_send.at[0], ag_recv.at[source],
            device_id=rank_peer(source), device_id_type=MESH,
        )

    near_first = sorted(range(1, nz), key=lambda d: min(d, nz - d))

    def shards_over_z():
        rs[rank] = gpart[rank]
        for d in range(1, nx * nc):
            shard_got(jnp.bitwise_xor(rank, d)).wait_recv()
        za[zi] = jnp.sum(rs[...], axis=0)
        if rounds:
            heard(len(rounds) - 1)
        for d in near_first:
            z_out(d).start()

    CH = 64
    nt = (((1,), (1,)), ((), ()))
    tn = (((0,), (0,)), ((), ()))
    nn = (((1,), (0,)), ((), ()))

    def arrived(h):
        to_partner(0, h).wait_recv()
        to_partner(1, h).wait_recv()
        forward(h).wait_recv()
        pltpu.make_async_copy(g_vm.at[h], g_vm.at[h], in_sem.at[h]).wait()

    slots = ((st0, dp0, tops0), (st1, dp1, tops1))

    PARTS = ((0, 2), (2, 4), (4, 5))

    def scores(h, slot, parts=PARTS):
        st, dp, tops = slots[slot]
        for lo, hi in parts:
            part = slice(lo * TOK, hi * TOK)
            raw = lax.dot_general(kv[h, 0], qr[h, part], nt, preferred_element_type=F32)
            st[:, part] = raw
            for j in range(lo, hi):
                cols = slice((j - lo) * TOK, (j - lo + 1) * TOK)
                top = jnp.full((8, TOK), -jnp.inf, F32)
                for c in range(LENGTH // CH):
                    rows = slice(c * CH, (c + 1) * CH)
                    masked = raw[rows, cols] + bias[rows, :]
                    top = jnp.maximum(top, jnp.max(masked.reshape(CH // 8, 8, TOK), axis=0))
                tops[j : j + 1, :] = jnp.max(top, axis=0, keepdims=True) * SCALE2
            dp[:, part] = lax.dot_general(kv[h, 1], g_vm[h, part], nt, preferred_element_type=F32)

    def softmax(j, slot):
        st, dp, tops = slots[slot]
        cols = slice(j * TOK, (j + 1) * TOK)
        top = tops[j : j + 1, :]
        weight = jnp.zeros((8, TOK), F32)
        delta = jnp.zeros((8, TOK), F32)
        for c in range(LENGTH // CH):
            rows = slice(c * CH, (c + 1) * CH)
            p = jnp.exp2((st[rows, cols] + bias[rows, :]) * SCALE2 - top)
            st[rows, cols] = p
            weight = weight + jnp.sum(p.reshape(CH // 8, 8, TOK), axis=0)
            delta = delta + jnp.sum((p * dp[rows, cols]).reshape(CH // 8, 8, TOK), axis=0)
        norm = 1.0 / jnp.sum(weight, axis=0, keepdims=True)
        delta = jnp.sum(delta, axis=0, keepdims=True) * norm
        for c in range(LENGTH // CH):
            rows = slice(c * CH, (c + 1) * CH)
            p = st[rows, cols] * norm
            pt[rows, cols] = p.astype(BF16)
            ds[rows, cols] = (p * (dp[rows, cols] - delta)).astype(BF16)

    def query_grads(h):
        dq = lax.dot_general(ds[...], kv[h, 0], tn, preferred_element_type=F32)
        along = jnp.zeros((TOK, HEAD_SIZE), F32)
        for j in range(HEADS_PER):
            d_part = dq[j * TOK : (j + 1) * TOK]
            d_part = d_part * cq[...] - swap_halves(d_part) * sq[...]
            dqw[h, j * TOK : (j + 1) * TOK] = d_part
            d_part = d_part * q_vm[h, j * TOK : (j + 1) * TOK].astype(F32)
            gpart[h, j : j + 1, :] = jnp.sum(d_part * rqb[...], axis=0, keepdims=True)
            along = along + d_part * qg_ref[pl.ds(h * HEADS_PER + j, 1), :]
        inner[...] = inner[...] + along

    def key_grads(h):
        dk = lax.dot_general(ds[...], qr[h], nn, preferred_element_type=F32)
        dv = lax.dot_general(pt[...], g_vm[h], nn, preferred_element_type=F32)
        own[h, 0] = dk[0:TOK]
        mid[h, 0] = dk[TOK : 2 * TOK]
        sd[h, 0] = dk[2 * TOK :]
        total = jnp.zeros((8, HEAD_SIZE), F32)
        for c in range(4):
            rows = slice(c * TOK, (c + 1) * TOK)
            d_part = dk[rows]
            k_part = kv[h, 0, rows].astype(F32)
            d_part = d_part * cosk[rows] - swap_halves(d_part) * sink[rows]
            k_part = k_part * cosk[rows] - swap_halves(k_part) * sink[rows]
            total = total + jnp.sum((d_part * k_part).reshape(TOK // 8, 8, HEAD_SIZE), axis=0)
        gpart[h, HEADS_PER : HEADS_PER + 1, :] = (
            jnp.sum(total, axis=0, keepdims=True) * SCALE / kg_ref[pl.ds(h, 1), :]
        )
        gpart[h, HEADS_PER + 1 :, :] = jnp.zeros((7 - HEADS_PER, HEAD_SIZE), F32)

        own[h, 1] = dv[0:TOK]
        mid[h, 1] = dv[TOK : 2 * TOK]
        sd[h, 1] = dv[2 * TOK :]

    def step(h, slot, first=None, last=False):
        if first is None:
            add_and_send(h - 2)
        else:
            @pl.when(jnp.logical_not(first))
            def _():
                add_and_send(h - 2)

        if not last:
            arrived(h + 1)
            if not isinstance(h, int):
                take(h + 2)
        for lo, hi in PARTS:
            if not last:
                scores(h + 1, 1 - slot, ((lo, hi),))
            for j in range(lo, hi):
                softmax(j, slot)
        query_grads(h)
        key_grads(h)
        @pl.when(rank != h)
        def _():
            shard_out(h).start()

        grads_to_partner(h).start()

    for h in range(2):
        take(h)
    arrived(0)
    scores(0, 0)

    last = KEY_VALUE_HEADS - 1

    @pl.loop(0, last // 2)
    def _(i):
        for r in range(1, len(rounds)):
            @pl.when(i == r)
            def _():
                heard(r - 1)
                tell(r)

        step(2 * i, 0, first=i == 0)
        step(2 * i + 1, 1, first=i == 0)

    step(last - 1, 0)
    step(last, 1, last=True)
    add_and_send(last - 1)
    shards_over_z()

    add_and_send(last)

    inner_q = jnp.sum(inner[...], axis=1, keepdims=True) * (1.0 / (QUERY_HEADS * HEAD_SIZE))
    cube = rqb[...] * rqb[...] * rqb[...] * inner_q
    inner[...] = cube

    def q_out(h, j):
        cols = pl.ds(pl.multiple_of((h * HEADS_PER + j) * HEAD_SIZE, HEAD_SIZE), HEAD_SIZE)
        rows = pl.ds(j * TOK, TOK)
        return pltpu.make_async_copy(outb.at[h, rows], qgrad_hbm.at[:, cols], out_sem.at[h, j])

    @pl.loop(0, KEY_VALUE_HEADS)
    def _(h):
        for j in range(HEADS_PER):
            rows = slice(j * TOK, (j + 1) * TOK)
            x = q_vm[h, rows].astype(F32)
            weighted = dqw[h, rows] * qg_ref[pl.ds(h * HEADS_PER + j, 1), :]
            outb[h, rows] = (rqb[...] * weighted - x * inner[...]).astype(BF16)
            q_out(h, j).start()

    for d in range(1, nz):
        z_got(d).wait_recv()
    ag[rank] = jnp.sum(za[...], axis=0)
    for d in range(1, nx * nc):
        total_out(d).start()

    def k_out(h, s, out):
        cols = pl.ds(pl.multiple_of(h * HEAD_SIZE, HEAD_SIZE), HEAD_SIZE)
        return pltpu.make_async_copy(si.at[h, s], out.at[:, cols], out_sem.at[h, HEADS_PER + s])

    inner[...] = jnp.zeros((TOK, HEAD_SIZE), F32)

    @pl.loop(0, KEY_VALUE_HEADS)
    def _(h):
        grads_across(h).wait()
        d_part = own[h, 0] + rd[h, 0, 0:TOK] + ri[h, 0].astype(F32)
        d_part = d_part * cq[...] - swap_halves(d_part) * sq[...]
        weighted = d_part * kg_ref[pl.ds(h, 1), :]
        dkw[h] = weighted
        inner[...] = inner[...] + weighted * k_vm[h].astype(F32)
        si[h, 1] = (own[h, 1] + rd[h, 1, 0:TOK] + ri[h, 1].astype(F32)).astype(BF16)
        k_out(h, 1, vgrad_hbm).start()

    inner_k = jnp.sum(inner[...], axis=1, keepdims=True) * (1.0 / (KEY_VALUE_HEADS * HEAD_SIZE))
    inner[...] = rkb[...] * rkb[...] * rkb[...] * inner_k

    @pl.loop(0, KEY_VALUE_HEADS)
    def _(h):
        si[h, 0] = (rkb[...] * dkw[h] - k_vm[h].astype(F32) * inner[...]).astype(BF16)
        k_out(h, 0, kgrad_hbm).start()

    for source in range(KEY_VALUE_HEADS):
        @pl.when(rank != source)
        def _():
            total_got(source).wait_recv()

        qgain_ref[source * HEADS_PER : (source + 1) * HEADS_PER, :] = ag[source, 0:HEADS_PER, :]
        kgain_ref[source : source + 1, :] = ag[source, HEADS_PER : HEADS_PER + 1, :]

    @pl.loop(0, KEY_VALUE_HEADS)
    def _(h):
        for s in range(2):
            to_across(s, h).wait_send()
            to_partner(s, h).wait_send()
        forward(h).wait_send()
        grads_to_partner(h).wait_send()
        for j in range(HEADS_PER):
            q_out(h, j).wait()
        k_out(h, 0, kgrad_hbm).wait()
        k_out(h, 1, vgrad_hbm).wait()

    for h in range(KEY_VALUE_HEADS):
        @pl.when(rank != h)
        def _():
            shard_out(h).wait_send()
    for d in range(1, nx * nc):
        total_out(d).wait_send()
    for d in range(1, nz):
        z_out(d).wait_send()


def settle(*refs):
    copies = [
        pltpu.make_async_copy(refs[i], refs[5 + i], refs[10].at[i]) for i in range(5)
    ]
    for copy in copies:
        copy.start()
    for copy in copies:
        copy.wait()


def body(nx, nz, nc, query_proj, key_proj, values, grad_out, query_gain, key_gain, segments, layout):
    cos_table, sin_table = rope_tables()
    assert nx * nc == KEY_VALUE_HEADS
    kvh, hs = KEY_VALUE_HEADS, HEAD_SIZE
    any_spec = pl.BlockSpec(memory_space=pl.ANY)
    vm_spec = pl.BlockSpec(memory_space=pltpu.VMEM)
    dma = pltpu.SemaphoreType.DMA
    out = pl.pallas_call(
        functools.partial(kernel, nx, nz, nc),
        out_shape=(
            jax.ShapeDtypeStruct(query_proj.shape, BF16),
            jax.ShapeDtypeStruct(key_proj.shape, BF16),
            jax.ShapeDtypeStruct(values.shape, BF16),
            jax.ShapeDtypeStruct((QUERY_HEADS, hs), F32),
            jax.ShapeDtypeStruct((kvh, hs), F32),
        ),
        in_specs=[pl.BlockSpec(memory_space=pltpu.HBM)] * 7 + [vm_spec] * 2 + [pl.BlockSpec(memory_space=pltpu.SMEM)],
        out_specs=(any_spec, any_spec, any_spec, vm_spec, vm_spec),
        scratch_shapes=[
            pltpu.VMEM((LENGTH, hs), F32),
            pltpu.VMEM((LENGTH, hs), F32),
            pltpu.VMEM((segments.shape[0] // TOK, TOK), jnp.int32),
            pltpu.VMEM((kvh, QROWS, hs), BF16),
            pltpu.VMEM((kvh, QROWS, hs), BF16),
            pltpu.VMEM((kvh, TOK, hs), BF16),
            pltpu.VMEM((kvh, 2, LENGTH, hs), BF16),
            pltpu.VMEM((kvh, QROWS, hs), BF16),
            pltpu.VMEM((LENGTH, QROWS), F32),
            pltpu.VMEM((LENGTH, QROWS), F32),
            pltpu.VMEM((LENGTH, QROWS), F32),
            pltpu.VMEM((LENGTH, QROWS), F32),
            pltpu.VMEM((LENGTH, QROWS), BF16),
            pltpu.VMEM((LENGTH, QROWS), BF16),
            pltpu.VMEM((kvh, QROWS, hs), F32),
            pltpu.VMEM((kvh, TOK, hs), F32),
            pltpu.VMEM((LENGTH, TOK), F32),
            pltpu.VMEM((LENGTH, TOK), F32),
            pltpu.VMEM((LENGTH, hs), F32),
            pltpu.VMEM((LENGTH, hs), F32),
            pltpu.VMEM((TOK, hs), F32),
            pltpu.VMEM((TOK, hs), F32),
            pltpu.VMEM((TOK, hs), F32),
            pltpu.VMEM((TOK, hs), F32),
            pltpu.VMEM((TOK, hs), F32),
            pltpu.VMEM((kvh, 2, TOK, hs), F32),
            pltpu.VMEM((kvh, 2, TOK, hs), F32),
            pltpu.VMEM((kvh, 2, 2 * TOK, hs), F32),
            pltpu.VMEM((kvh, 2, 2 * TOK, hs), F32),
            pltpu.VMEM((kvh, 2, TOK, hs), BF16),
            pltpu.VMEM((kvh, 2, TOK, hs), BF16),
            pltpu.VMEM((kvh, QROWS, hs), BF16),
            pltpu.VMEM((8, TOK), F32),
            pltpu.VMEM((8, TOK), F32),
            pltpu.VMEM((kvh, 8, hs), F32),
            pltpu.VMEM((kvh, 8, hs), F32),
            pltpu.VMEM((nz, 8, hs), F32),
            pltpu.VMEM((kvh, 8, hs), F32),
            dma((kvh,)), dma((2,)), dma((kvh,)), dma((3,)),
            dma((2, kvh)), dma((2, kvh)), dma((2, kvh)), dma((2, kvh)), dma((kvh,)), dma((kvh,)),
            dma((kvh,)), dma((kvh,)), dma((kvh,)), dma((kvh,)),
            dma((kvh,)), dma((kvh,)), dma((nz,)), dma((nz,)), dma((kvh,)), dma((kvh,)),
            pltpu.SemaphoreType.REGULAR((3, 2)),
            dma((kvh, HEADS_PER + 2)),
        ],
        compiler_params=pltpu.CompilerParams(
            collective_id=0, has_side_effects=True, vmem_limit_bytes=36 * 1024 * 1024
        ),
    )(
        *(
            pltpu.with_memory_space_constraint(x, pltpu.HBM)
            for x in (
                query_proj, key_proj, values, grad_out,
                jnp.asarray(cos_table), jnp.asarray(sin_table), segments.reshape(-1, TOK),
                query_gain.reshape(QUERY_HEADS, hs), key_gain.reshape(kvh, hs), layout,
            )
        ),
    )
    out = pl.pallas_call(
        settle,
        out_shape=[jax.ShapeDtypeStruct(o.shape, o.dtype) for o in out],
        in_specs=[any_spec] * 5,
        out_specs=[any_spec] * 5,
        scratch_shapes=[dma((5,))],
        compiler_params=pltpu.CompilerParams(vmem_limit_bytes=1024 * 1024),
    )(*out)
    return out[0], out[1], out[2], out[3].reshape(-1), out[4].reshape(-1)


def solution(mesh):
    nx, nz, nc = 4, 16, 2
    split = Mesh(mesh.devices.reshape(mesh.shape["groups"], nx, nz, nc), GROUPS_CONTEXT)
    tokens = P(GROUPS_CONTEXT, None)
    return jax.shard_map(
        functools.partial(body, nx, nz, nc),
        mesh=split,
        in_specs=(tokens, tokens, tokens, tokens, P(), P(), P("groups"), P("groups")),
        out_specs=(tokens, tokens, tokens, P("groups"), P("groups")),
        check_vma=False,
    )
```

```python
import functools
import math

import jax
import jax.numpy as jnp
import numpy as np
from jax import lax
from jax.experimental import pallas as pl
from jax.experimental.pallas import tpu as pltpu
from jax.sharding import Mesh
from jax.sharding import PartitionSpec as P

QUERY_HEADS = 40
KEY_VALUE_HEADS = 8
HEADS_PER = QUERY_HEADS // KEY_VALUE_HEADS
HEAD_SIZE = 128
SPAN = 64
LENGTH = 512
SPANS = LENGTH // SPAN
TOK = 128
QROWS = HEADS_PER * TOK
CONTEXT = ("context_0", "context_1", "context_2")
GROUPS_CONTEXT = ("groups", "context_0", "context_1", "context_2")
NORM_EPS = 1e-06
ROPE_BASE = 500000.0
SCALE = HEAD_SIZE ** (-0.5)
SCALE2 = SCALE * math.log2(math.e)
MESH = pl.DeviceIdType.MESH
F32 = jnp.float32
BF16 = jnp.bfloat16


def rope_tables():
    half = HEAD_SIZE // 2
    inv_freq = np.power(ROPE_BASE, -2.0 * np.arange(half) / HEAD_SIZE)
    angles = np.arange(LENGTH)[:, None] * inv_freq[None, :]
    cosine, sine = np.cos(angles), np.sin(angles)
    return (
        np.concatenate([cosine, cosine], axis=1).astype(np.float32),
        np.concatenate([-sine, sine], axis=1).astype(np.float32),
    )


def swap_halves(x):
    return pltpu.roll(x, HEAD_SIZE // 2, 1)


def kernel(
    nx, nz, nc,
    q_hbm, k_hbm, v_hbm, g_hbm, cos_hbm, sin_hbm, seg_hbm, qg_ref, kg_ref, lay_ref,
    qgrad_hbm, kgrad_hbm, vgrad_hbm, qgain_ref, kgain_ref,
    cos_ref, sin_ref, seg_ref,
    q_vm, g_vm, k_vm, kv, qr, st0, st1, dp0, dp1, pt, ds, dqw, dkw,
    bias, segcol, cosk, sink, cq, sq, rqb, rkb, inner,
    own, mid, sd, rd, si, ri, outb,
    tops0, tops1, gpart, rs, za, ag,
    in_sem, kin_sem, vin_sem, tab_sem,
    z_send, z_recv, c_send, c_recv, f_send, f_recv,
    d_send, d_recv, i_send, i_recv,
    rs_send, rs_recv, za_send, za_recv, ag_send, ag_recv, near_sem,
    out_sem,
):
    xi = lax.axis_index("context_0")
    zi = lax.axis_index("context_1")
    ci = lax.axis_index("context_2")
    rank = xi * nc + ci
    seq = xi * (nz // 2) + zi // 2
    z_flip = zi + 1 - 2 * lax.rem(zi, 2)
    partner = {"context_2": 1 - ci}
    across = {"context_1": z_flip}

    def rank_peer(other):
        return {"context_0": other // nc, "context_2": lax.rem(other, nc)}

    def k_in(h):
        cols = pl.ds(pl.multiple_of(h * HEAD_SIZE, HEAD_SIZE), HEAD_SIZE)
        return pltpu.make_async_copy(k_hbm.at[:, cols], k_vm.at[h], kin_sem.at[0])

    def v_in(h):
        cols = pl.ds(pl.multiple_of(h * HEAD_SIZE, HEAD_SIZE), HEAD_SIZE)
        return pltpu.make_async_copy(v_hbm.at[:, cols], kv.at[h, 1, 0:TOK], vin_sem.at[h])

    def q_in(h, j):
        cols = pl.ds(pl.multiple_of((h * HEADS_PER + j) * HEAD_SIZE, HEAD_SIZE), HEAD_SIZE)
        rows = pl.ds(j * TOK, TOK)
        return pltpu.make_async_copy(q_hbm.at[:, cols], q_vm.at[h, rows], kin_sem.at[1])

    def g_in(h, j):
        cols = pl.ds(pl.multiple_of((h * HEADS_PER + j) * HEAD_SIZE, HEAD_SIZE), HEAD_SIZE)
        rows = pl.ds(j * TOK, TOK)
        return pltpu.make_async_copy(g_hbm.at[:, cols], g_vm.at[h, rows], in_sem.at[h])

    tables = [
        pltpu.make_async_copy(source, target, tab_sem.at[index])
        for index, (source, target) in enumerate(
            ((cos_hbm, cos_ref), (sin_hbm, sin_ref), (seg_hbm, seg_ref))
        )
    ]
    for h in range(KEY_VALUE_HEADS):
        v_in(h).start()
        k_in(h).start()
    for table in tables:
        table.start()

    barrier = pltpu.get_barrier_semaphore()
    for d in range(1, nx * nc):
        pl.semaphore_signal(
            barrier, inc=1, device_id=rank_peer(jnp.bitwise_xor(rank, d)), device_id_type=MESH
        )
    sides = sorted({1, nz - 1})
    for d in sides:
        pl.semaphore_signal(
            barrier, inc=1, device_id={"context_1": lax.rem(zi + d, nz)}, device_id_type=MESH
        )

    rounds = [1 << r for r in range(8) if 1 << r < nz // 2]

    def tell(r):
        for side, d in enumerate((rounds[r], nz - rounds[r])):
            pl.semaphore_signal(
                near_sem.at[r, side], inc=1,
                device_id={"context_1": lax.rem(zi + d, nz)}, device_id_type=MESH,
            )

    def heard(r):
        for side in range(2):
            pl.semaphore_wait(near_sem.at[r, side], 1)


    my_local = 2 * lax.rem(zi, 2) + ci
    sub_iota = lax.broadcasted_iota(jnp.int32, (SPAN, TOK), 0)
    lane = lax.broadcasted_iota(jnp.int32, (8, TOK), 1)
    spans = []
    for flip in (0, 2, 1, 3):
        holder = jnp.bitwise_xor(my_local, flip)
        for part in range(2):
            slot = lay_ref[seq * SPANS + 2 * holder + part]
            spans.append(jnp.bitwise_and(jnp.full((8, TOK), slot, jnp.int32), SPANS - 1))

    def pick(span, table):
        chosen = table[0:SPAN, :]
        wide = jnp.concatenate([span] * (SPAN // 8), axis=0)
        for at in range(1, SPANS):
            chosen = jnp.where(wide == at, table[at * SPAN : (at + 1) * SPAN, :], chosen)
        return chosen

    def key_rotary(index):
        rows = slice(index * SPAN, (index + 1) * SPAN)
        cosk[rows, :] = pick(spans[index], cos_ref)
        sink[rows, :] = pick(spans[index], sin_ref)

    def to_across(s, h):
        return pltpu.make_async_remote_copy(
            kv.at[h, s, 0:TOK], kv.at[h, s, TOK : 2 * TOK], z_send.at[s, h], z_recv.at[s, h],
            device_id=across, device_id_type=MESH,
        )

    def to_partner(s, h):
        return pltpu.make_async_remote_copy(
            kv.at[h, s, 0:TOK], kv.at[h, s, 2 * TOK : 3 * TOK], c_send.at[s, h], c_recv.at[s, h],
            device_id=partner, device_id_type=MESH,
        )

    def forward(h):
        return pltpu.make_async_remote_copy(
            kv.at[h, :, TOK : 2 * TOK], kv.at[h, :, 3 * TOK : 4 * TOK], f_send.at[h], f_recv.at[h],
            device_id=partner, device_id_type=MESH,
        )

    def grads_to_partner(h):
        return pltpu.make_async_remote_copy(
            sd.at[h], rd.at[h], d_send.at[h], d_recv.at[h],
            device_id=partner, device_id_type=MESH,
        )

    def grads_across(h):
        return pltpu.make_async_remote_copy(
            si.at[h], ri.at[h], i_send.at[h], i_recv.at[h],
            device_id=across, device_id_type=MESH,
        )

    def values_out(h):
        v_in(h).wait()
        to_across(1, h).start()
        to_partner(1, h).start()

    AHEAD = 2
    pl.semaphore_wait(barrier, nx * nc - 1 + len(sides))
    if rounds:
        tell(0)
    for h in range(AHEAD):
        values_out(h)

    @pl.loop(0, KEY_VALUE_HEADS)
    def _(h):
        for j in range(HEADS_PER):
            q_in(h, j).start()
            g_in(h, j).start()

    pltpu.make_async_copy(k_vm, k_vm, kin_sem.at[0]).wait()
    acc = jnp.zeros((TOK, HEAD_SIZE), F32)
    for h in range(KEY_VALUE_HEADS):
        x = k_vm[h].astype(F32)
        acc = acc + x * x
    mean_sq = jnp.sum(acc, axis=1, keepdims=True) * (1.0 / (KEY_VALUE_HEADS * HEAD_SIZE))
    rkb[...] = jnp.broadcast_to(lax.rsqrt(mean_sq + NORM_EPS), (TOK, HEAD_SIZE))
    for table in tables:
        table.wait()
    key_rotary(0)
    key_rotary(1)

    @pl.loop(0, KEY_VALUE_HEADS)
    def _(h):
        normed = k_vm[h].astype(F32) * rkb[...] * kg_ref[pl.ds(h, 1), :]
        kv[h, 0, 0:TOK] = (normed * cosk[0:TOK] + swap_halves(normed) * sink[0:TOK]).astype(BF16)
        to_across(0, h).start()
        to_partner(0, h).start()

        @pl.when(h < KEY_VALUE_HEADS - AHEAD)
        def _():
            values_out(h + AHEAD)

    cq[...] = cosk[0:TOK] * SCALE
    sq[...] = sink[0:TOK] * SCALE
    for index in range(2, SPANS):
        key_rotary(index)

    first = lane < SPAN
    query_span = jnp.where(first, spans[0], spans[1])
    doc_row = jnp.zeros((8, TOK), F32)
    for part in range(LENGTH // TOK):
        row = seg_ref[pl.ds(seq * (LENGTH // TOK) + part, 1), :].astype(F32)
        segcol[part * TOK : (part + 1) * TOK, :] = jnp.transpose(
            jnp.broadcast_to(row, (TOK, TOK))
        )
        row = jnp.broadcast_to(row, (8, TOK))
        turned = pltpu.roll(row, SPAN, 1)
        doc_row = jnp.where(query_span == 2 * part, jnp.where(first, row, turned), doc_row)
        doc_row = jnp.where(query_span == 2 * part + 1, jnp.where(first, turned, row), doc_row)
    doc_row = doc_row[0:1, :]
    pos_row = (query_span * SPAN + jnp.bitwise_and(lane, SPAN - 1))[0:1, :]
    for index, span in enumerate(spans):
        doc_col = pick(span, segcol)
        pos_col = span[0:1, :] * SPAN + sub_iota
        allowed = (doc_col == doc_row) & (pos_col <= pos_row)
        bias[index * SPAN : (index + 1) * SPAN, :] = jnp.where(allowed, 0.0, -jnp.inf)

    pltpu.make_async_copy(q_vm, q_vm, kin_sem.at[1]).wait()
    inner[...] = jnp.zeros((TOK, HEAD_SIZE), F32)

    @pl.loop(0, KEY_VALUE_HEADS)
    def _(h):
        total = inner[...]
        for j in range(HEADS_PER):
            x = q_vm[h, j * TOK : (j + 1) * TOK].astype(F32)
            total = total + x * x
        inner[...] = total

    mean_sq = jnp.sum(inner[...], axis=1, keepdims=True) * (1.0 / (QUERY_HEADS * HEAD_SIZE))
    rqb[...] = jnp.broadcast_to(lax.rsqrt(mean_sq + NORM_EPS), (TOK, HEAD_SIZE))
    inner[...] = jnp.zeros((TOK, HEAD_SIZE), F32)

    def take(h):
        to_across(0, h).wait_recv()
        to_across(1, h).wait_recv()
        forward(h).start()

    take(0)

    @pl.loop(0, KEY_VALUE_HEADS)
    def _(h):
        for j in range(HEADS_PER):
            rows = slice(j * TOK, (j + 1) * TOK)
            normed = q_vm[h, rows].astype(F32) * rqb[...] * qg_ref[pl.ds(h * HEADS_PER + j, 1), :]
            qr[h, rows] = (
                normed * cosk[0:TOK] + swap_halves(normed) * sink[0:TOK]
            ).astype(BF16)

    def add_and_send(h):
        grads_to_partner(h).wait_recv()
        for s in range(2):
            si[h, s] = (mid[h, s] + rd[h, s, TOK : 2 * TOK]).astype(BF16)
        grads_across(h).start()

    def shard_out(h):
        return pltpu.make_async_remote_copy(
            gpart.at[h], rs.at[rank], rs_send.at[h], rs_recv.at[rank],
            device_id=rank_peer(h), device_id_type=MESH,
        )

    def shard_got(source):
        return pltpu.make_async_remote_copy(
            gpart.at[0], rs.at[source], rs_send.at[0], rs_recv.at[source],
            device_id=rank_peer(source), device_id_type=MESH,
        )

    def z_copy(buffer, send, recv, d, source):
        return pltpu.make_async_remote_copy(
            buffer.at[source], buffer.at[source], send.at[d], recv.at[source],
            device_id={"context_1": lax.rem(zi + d, nz)}, device_id_type=MESH,
        )

    def z_out(d):
        return z_copy(za, za_send, za_recv, d, zi)

    def z_got(d):
        return z_copy(za, za_send, za_recv, d, lax.rem(zi + d, nz))

    def total_out(d):
        other = jnp.bitwise_xor(rank, d)
        return pltpu.make_async_remote_copy(
            ag.at[rank], ag.at[rank], ag_send.at[d], ag_recv.at[rank],
            device_id=rank_peer(other), device_id_type=MESH,
        )

    def total_got(source):
        return pltpu.make_async_remote_copy(
            ag.at[source], ag.at[source], ag_send.at[0], ag_recv.at[source],
            device_id=rank_peer(source), device_id_type=MESH,
        )

    near_first = sorted(range(1, nz), key=lambda d: min(d, nz - d))

    def shards_over_z():
        rs[rank] = gpart[rank]
        for d in range(1, nx * nc):
            shard_got(jnp.bitwise_xor(rank, d)).wait_recv()
        za[zi] = jnp.sum(rs[...], axis=0)
        if rounds:
            heard(len(rounds) - 1)
        for d in near_first:
            z_out(d).start()

    CH = 64
    nt = (((1,), (1,)), ((), ()))
    tn = (((0,), (0,)), ((), ()))
    nn = (((1,), (0,)), ((), ()))

    def arrived(h):
        to_partner(0, h).wait_recv()
        to_partner(1, h).wait_recv()
        forward(h).wait_recv()
        pltpu.make_async_copy(g_vm.at[h], g_vm.at[h], in_sem.at[h]).wait()

    slots = ((st0, dp0, tops0), (st1, dp1, tops1))

    PARTS = ((0, 2), (2, 4), (4, 5))

    def scores(h, slot, parts=PARTS):
        st, dp, tops = slots[slot]
        for lo, hi in parts:
            part = slice(lo * TOK, hi * TOK)
            raw = lax.dot_general(kv[h, 0], qr[h, part], nt, preferred_element_type=F32)
            st[:, part] = raw
            for j in range(lo, hi):
                cols = slice((j - lo) * TOK, (j - lo + 1) * TOK)
                top = jnp.full((8, TOK), -jnp.inf, F32)
                for c in range(LENGTH // CH):
                    rows = slice(c * CH, (c + 1) * CH)
                    masked = raw[rows, cols] + bias[rows, :]
                    top = jnp.maximum(top, jnp.max(masked.reshape(CH // 8, 8, TOK), axis=0))
                tops[j : j + 1, :] = jnp.max(top, axis=0, keepdims=True) * SCALE2
            dp[:, part] = lax.dot_general(kv[h, 1], g_vm[h, part], nt, preferred_element_type=F32)

    def softmax(j, slot):
        st, dp, tops = slots[slot]
        cols = slice(j * TOK, (j + 1) * TOK)
        top = tops[j : j + 1, :]
        weight = jnp.zeros((8, TOK), F32)
        delta = jnp.zeros((8, TOK), F32)
        for c in range(LENGTH // CH):
            rows = slice(c * CH, (c + 1) * CH)
            p = jnp.exp2((st[rows, cols] + bias[rows, :]) * SCALE2 - top)
            st[rows, cols] = p
            weight = weight + jnp.sum(p.reshape(CH // 8, 8, TOK), axis=0)
            delta = delta + jnp.sum((p * dp[rows, cols]).reshape(CH // 8, 8, TOK), axis=0)
        norm = 1.0 / jnp.sum(weight, axis=0, keepdims=True)
        delta = jnp.sum(delta, axis=0, keepdims=True) * norm
        for c in range(LENGTH // CH):
            rows = slice(c * CH, (c + 1) * CH)
            p = st[rows, cols] * norm
            pt[rows, cols] = p.astype(BF16)
            ds[rows, cols] = (p * (dp[rows, cols] - delta)).astype(BF16)

    def query_grads(h):
        dq = lax.dot_general(ds[...], kv[h, 0], tn, preferred_element_type=F32)
        along = jnp.zeros((TOK, HEAD_SIZE), F32)
        for j in range(HEADS_PER):
            d_part = dq[j * TOK : (j + 1) * TOK]
            d_part = d_part * cq[...] - swap_halves(d_part) * sq[...]
            dqw[h, j * TOK : (j + 1) * TOK] = d_part
            d_part = d_part * q_vm[h, j * TOK : (j + 1) * TOK].astype(F32)
            gpart[h, j : j + 1, :] = jnp.sum(d_part * rqb[...], axis=0, keepdims=True)
            along = along + d_part * qg_ref[pl.ds(h * HEADS_PER + j, 1), :]
        inner[...] = inner[...] + along

    def key_grads(h):
        dk = lax.dot_general(ds[...], qr[h], nn, preferred_element_type=F32)
        dv = lax.dot_general(pt[...], g_vm[h], nn, preferred_element_type=F32)
        own[h, 0] = dk[0:TOK]
        mid[h, 0] = dk[TOK : 2 * TOK]
        sd[h, 0] = dk[2 * TOK :]
        total = jnp.zeros((8, HEAD_SIZE), F32)
        for c in range(4):
            rows = slice(c * TOK, (c + 1) * TOK)
            d_part = dk[rows]
            k_part = kv[h, 0, rows].astype(F32)
            d_part = d_part * cosk[rows] - swap_halves(d_part) * sink[rows]
            k_part = k_part * cosk[rows] - swap_halves(k_part) * sink[rows]
            total = total + jnp.sum((d_part * k_part).reshape(TOK // 8, 8, HEAD_SIZE), axis=0)
        gpart[h, HEADS_PER : HEADS_PER + 1, :] = (
            jnp.sum(total, axis=0, keepdims=True) * SCALE / kg_ref[pl.ds(h, 1), :]
        )
        gpart[h, HEADS_PER + 1 :, :] = jnp.zeros((7 - HEADS_PER, HEAD_SIZE), F32)

        own[h, 1] = dv[0:TOK]
        mid[h, 1] = dv[TOK : 2 * TOK]
        sd[h, 1] = dv[2 * TOK :]

    def step(h, slot, first=None, last=False):
        if first is None:
            add_and_send(h - 2)
        else:
            @pl.when(jnp.logical_not(first))
            def _():
                add_and_send(h - 2)

        if not last:
            arrived(h + 1)
            if not isinstance(h, int):
                take(h + 2)
        for lo, hi in PARTS:
            if not last:
                scores(h + 1, 1 - slot, ((lo, hi),))
            for j in range(lo, hi):
                softmax(j, slot)
        query_grads(h)
        key_grads(h)
        @pl.when(rank != h)
        def _():
            shard_out(h).start()

        grads_to_partner(h).start()

    take(1)
    arrived(0)
    scores(0, 0)

    last = KEY_VALUE_HEADS - 1

    @pl.loop(0, last // 2)
    def _(i):
        for r in range(1, len(rounds)):
            @pl.when(i == r)
            def _():
                heard(r - 1)
                tell(r)

        step(2 * i, 0, first=i == 0)
        step(2 * i + 1, 1, first=i == 0)

    step(last - 1, 0)
    step(last, 1, last=True)
    add_and_send(last - 1)
    shards_over_z()

    add_and_send(last)

    inner_q = jnp.sum(inner[...], axis=1, keepdims=True) * (1.0 / (QUERY_HEADS * HEAD_SIZE))
    cube = rqb[...] * rqb[...] * rqb[...] * inner_q
    inner[...] = cube

    def q_out(h, j):
        cols = pl.ds(pl.multiple_of((h * HEADS_PER + j) * HEAD_SIZE, HEAD_SIZE), HEAD_SIZE)
        rows = pl.ds(j * TOK, TOK)
        return pltpu.make_async_copy(outb.at[h, rows], qgrad_hbm.at[:, cols], out_sem.at[h, j])

    @pl.loop(0, KEY_VALUE_HEADS)
    def _(h):
        for j in range(HEADS_PER):
            rows = slice(j * TOK, (j + 1) * TOK)
            x = q_vm[h, rows].astype(F32)
            weighted = dqw[h, rows] * qg_ref[pl.ds(h * HEADS_PER + j, 1), :]
            outb[h, rows] = (rqb[...] * weighted - x * inner[...]).astype(BF16)
            q_out(h, j).start()

    for d in range(1, nz):
        z_got(d).wait_recv()
    ag[rank] = jnp.sum(za[...], axis=0)
    for d in range(1, nx * nc):
        total_out(d).start()

    def k_out(h, s, out):
        cols = pl.ds(pl.multiple_of(h * HEAD_SIZE, HEAD_SIZE), HEAD_SIZE)
        return pltpu.make_async_copy(si.at[h, s], out.at[:, cols], out_sem.at[h, HEADS_PER + s])

    inner[...] = jnp.zeros((TOK, HEAD_SIZE), F32)

    @pl.loop(0, KEY_VALUE_HEADS)
    def _(h):
        grads_across(h).wait()
        d_part = own[h, 0] + rd[h, 0, 0:TOK] + ri[h, 0].astype(F32)
        d_part = d_part * cq[...] - swap_halves(d_part) * sq[...]
        weighted = d_part * kg_ref[pl.ds(h, 1), :]
        dkw[h] = weighted
        inner[...] = inner[...] + weighted * k_vm[h].astype(F32)
        si[h, 1] = (own[h, 1] + rd[h, 1, 0:TOK] + ri[h, 1].astype(F32)).astype(BF16)
        k_out(h, 1, vgrad_hbm).start()

    inner_k = jnp.sum(inner[...], axis=1, keepdims=True) * (1.0 / (KEY_VALUE_HEADS * HEAD_SIZE))
    inner[...] = rkb[...] * rkb[...] * rkb[...] * inner_k

    @pl.loop(0, KEY_VALUE_HEADS)
    def _(h):
        si[h, 0] = (rkb[...] * dkw[h] - k_vm[h].astype(F32) * inner[...]).astype(BF16)
        k_out(h, 0, kgrad_hbm).start()

    for source in range(KEY_VALUE_HEADS):
        @pl.when(rank != source)
        def _():
            total_got(source).wait_recv()

        qgain_ref[source * HEADS_PER : (source + 1) * HEADS_PER, :] = ag[source, 0:HEADS_PER, :]
        kgain_ref[source : source + 1, :] = ag[source, HEADS_PER : HEADS_PER + 1, :]

    @pl.loop(0, KEY_VALUE_HEADS)
    def _(h):
        for s in range(2):
            to_across(s, h).wait_send()
            to_partner(s, h).wait_send()
        forward(h).wait_send()
        grads_to_partner(h).wait_send()
        for j in range(HEADS_PER):
            q_out(h, j).wait()
        k_out(h, 0, kgrad_hbm).wait()
        k_out(h, 1, vgrad_hbm).wait()

    for h in range(KEY_VALUE_HEADS):
        @pl.when(rank != h)
        def _():
            shard_out(h).wait_send()
    for d in range(1, nx * nc):
        total_out(d).wait_send()
    for d in range(1, nz):
        z_out(d).wait_send()


def settle(*refs):
    copies = [
        pltpu.make_async_copy(refs[i], refs[5 + i], refs[10].at[i]) for i in range(5)
    ]
    for copy in copies:
        copy.start()
    for copy in copies:
        copy.wait()


def body(nx, nz, nc, query_proj, key_proj, values, grad_out, query_gain, key_gain, segments, layout):
    cos_table, sin_table = rope_tables()
    assert nx * nc == KEY_VALUE_HEADS
    kvh, hs = KEY_VALUE_HEADS, HEAD_SIZE
    any_spec = pl.BlockSpec(memory_space=pl.ANY)
    vm_spec = pl.BlockSpec(memory_space=pltpu.VMEM)
    dma = pltpu.SemaphoreType.DMA
    out = pl.pallas_call(
        functools.partial(kernel, nx, nz, nc),
        out_shape=(
            jax.ShapeDtypeStruct(query_proj.shape, BF16),
            jax.ShapeDtypeStruct(key_proj.shape, BF16),
            jax.ShapeDtypeStruct(values.shape, BF16),
            jax.ShapeDtypeStruct((QUERY_HEADS, hs), F32),
            jax.ShapeDtypeStruct((kvh, hs), F32),
        ),
        in_specs=[pl.BlockSpec(memory_space=pltpu.HBM)] * 7 + [vm_spec] * 2 + [pl.BlockSpec(memory_space=pltpu.SMEM)],
        out_specs=(any_spec, any_spec, any_spec, vm_spec, vm_spec),
        scratch_shapes=[
            pltpu.VMEM((LENGTH, hs), F32),
            pltpu.VMEM((LENGTH, hs), F32),
            pltpu.VMEM((segments.shape[0] // TOK, TOK), jnp.int32),
            pltpu.VMEM((kvh, QROWS, hs), BF16),
            pltpu.VMEM((kvh, QROWS, hs), BF16),
            pltpu.VMEM((kvh, TOK, hs), BF16),
            pltpu.VMEM((kvh, 2, LENGTH, hs), BF16),
            pltpu.VMEM((kvh, QROWS, hs), BF16),
            pltpu.VMEM((LENGTH, QROWS), F32),
            pltpu.VMEM((LENGTH, QROWS), F32),
            pltpu.VMEM((LENGTH, QROWS), F32),
            pltpu.VMEM((LENGTH, QROWS), F32),
            pltpu.VMEM((LENGTH, QROWS), BF16),
            pltpu.VMEM((LENGTH, QROWS), BF16),
            pltpu.VMEM((kvh, QROWS, hs), F32),
            pltpu.VMEM((kvh, TOK, hs), F32),
            pltpu.VMEM((LENGTH, TOK), F32),
            pltpu.VMEM((LENGTH, TOK), F32),
            pltpu.VMEM((LENGTH, hs), F32),
            pltpu.VMEM((LENGTH, hs), F32),
            pltpu.VMEM((TOK, hs), F32),
            pltpu.VMEM((TOK, hs), F32),
            pltpu.VMEM((TOK, hs), F32),
            pltpu.VMEM((TOK, hs), F32),
            pltpu.VMEM((TOK, hs), F32),
            pltpu.VMEM((kvh, 2, TOK, hs), F32),
            pltpu.VMEM((kvh, 2, TOK, hs), F32),
            pltpu.VMEM((kvh, 2, 2 * TOK, hs), F32),
            pltpu.VMEM((kvh, 2, 2 * TOK, hs), F32),
            pltpu.VMEM((kvh, 2, TOK, hs), BF16),
            pltpu.VMEM((kvh, 2, TOK, hs), BF16),
            pltpu.VMEM((kvh, QROWS, hs), BF16),
            pltpu.VMEM((8, TOK), F32),
            pltpu.VMEM((8, TOK), F32),
            pltpu.VMEM((kvh, 8, hs), F32),
            pltpu.VMEM((kvh, 8, hs), F32),
            pltpu.VMEM((nz, 8, hs), F32),
            pltpu.VMEM((kvh, 8, hs), F32),
            dma((kvh,)), dma((2,)), dma((kvh,)), dma((3,)),
            dma((2, kvh)), dma((2, kvh)), dma((2, kvh)), dma((2, kvh)), dma((kvh,)), dma((kvh,)),
            dma((kvh,)), dma((kvh,)), dma((kvh,)), dma((kvh,)),
            dma((kvh,)), dma((kvh,)), dma((nz,)), dma((nz,)), dma((kvh,)), dma((kvh,)),
            pltpu.SemaphoreType.REGULAR((3, 2)),
            dma((kvh, HEADS_PER + 2)),
        ],
        compiler_params=pltpu.CompilerParams(
            collective_id=0, has_side_effects=True, vmem_limit_bytes=36 * 1024 * 1024
        ),
    )(
        *(
            pltpu.with_memory_space_constraint(x, pltpu.HBM)
            for x in (
                query_proj, key_proj, values, grad_out,
                jnp.asarray(cos_table), jnp.asarray(sin_table), segments.reshape(-1, TOK),
                query_gain.reshape(QUERY_HEADS, hs), key_gain.reshape(kvh, hs), layout,
            )
        ),
    )
    out = pl.pallas_call(
        settle,
        out_shape=[jax.ShapeDtypeStruct(o.shape, o.dtype) for o in out],
        in_specs=[any_spec] * 5,
        out_specs=[any_spec] * 5,
        scratch_shapes=[dma((5,))],
        compiler_params=pltpu.CompilerParams(vmem_limit_bytes=1024 * 1024),
    )(*out)
    return out[0], out[1], out[2], out[3].reshape(-1), out[4].reshape(-1)


def solution(mesh):
    nx, nz, nc = 4, 16, 2
    split = Mesh(mesh.devices.reshape(mesh.shape["groups"], nx, nz, nc), GROUPS_CONTEXT)
    tokens = P(GROUPS_CONTEXT, None)
    return jax.shard_map(
        functools.partial(body, nx, nz, nc),
        mesh=split,
        in_specs=(tokens, tokens, tokens, tokens, P(), P(), P("groups"), P("groups")),
        out_specs=(tokens, tokens, tokens, P("groups"), P("groups")),
        check_vma=False,
    )
```
